256 devices in a mesh: ccd: 128 (over z, x, y), row: 2 (over core).
Axes of the slice: x: 4, y: 4, z: 8, core: 2. Of those that a mesh axis runs over, the one named last changes fastest.
Arguments:
- exposure: float32 [128, 48, 2048], P('ccd', 'row'), may hold values from -6 to 6
- row_shift: int32 [128], P('ccd'), may hold values from 0 to 7
- row_fraction: bfloat16 [128, 48], P('ccd', 'row'), may hold values from 0 to 1
- column_shift: int32 [128], P('ccd'), may hold values from 0 to 127
- column_fraction: bfloat16 [128, 2048], P('ccd'), may hold values from 0 to 1
- piece_width: int32 [128, 16], P('ccd'), may hold values from 1 to 128
- route_tile: int32 [128, 16], P('ccd'), may hold values from 0 to 127, as said below
- route_cell: int32 [128, 16], P('ccd'), may hold values from 0 to 31, as said below
- template: float32 [128, 48, 4096], P('ccd', 'row'), may hold values from -6 to 6
- match_kernel: bfloat16 [128, 41, 41], P('ccd'), may hold values from -0.15625 to 0.15625
- detection_kernel: bfloat16 [128, 15, 15], P('ccd'), may hold values from -0.375 to 0.375
Outputs:
- difference: float32 [128, 48, 4096], P('ccd', 'row')
- significance: float32 [128, 48, 4096], P('ccd', 'row')
- noise_level: float32 [], replicated
The draws below stay inside these ranges and needn't reach their ends.
Inputs may be any that keep to these rules, and one draw needn't show every extreme that they name: Piece p of CCD c lands on tile route_tile[c, p]. Every tile receives at least one piece and at most 32 pieces in all; a quarter of the tiles receive exactly 32. No CCD puts more than 2 pieces on one tile, and some CCDs put exactly 2. `route_cell`: pieces that land on one tile fill different cells.
All inputs are finite; a program needn't handle non-finite values.
Results may differ from the reference program's by a relative error of at most 0.0044.
Values may be sent and summed in bfloat16 or wider, within the bound.
A program may use at most 128 MiB of HBM per device.

```python
import jax
import jax.numpy as jnp
from jax import lax

W = 2048
PW = 128
NP = 16
CROWS = 48
CCDS = 128
NT = 128
CAP = 32
HALO = 8
KS = 41
DK = 15


def route_tables(key):
    key_order = jax.random.fold_in(key, 101)
    key_pattern = jax.random.fold_in(key, 102)
    key_piece = jax.random.fold_in(key, 103)
    key_cell = jax.random.fold_in(key, 104)
    groups = CCDS // 4
    spreads = jax.random.randint(key_pattern, (groups,), 0, NP // 2).astype(jnp.int32)
    loads = jnp.stack([jnp.full((groups,), 2 * NP, jnp.int32), NP - spreads, NP // 2 + spreads, jnp.full((groups,), NP - NP // 2, jnp.int32)], axis=1).reshape(-1).astype(jnp.int32)
    order = jax.random.permutation(key_order, CCDS).astype(jnp.int32)
    ends = jnp.cumsum(loads).astype(jnp.int32)
    token = jnp.arange(CCDS * NP, dtype=jnp.int32)
    position = jnp.searchsorted(ends, token, side='right').astype(jnp.int32)
    piece_rank = token - (ends[position] - loads[position])
    tile_flat = order[position]
    spots = jax.random.randint(key_cell, (CCDS, CAP), 0, 1 << 20).astype(jnp.int32) * CAP + jnp.arange(CAP, dtype=jnp.int32)[None, :]
    cell_order = jnp.argsort(spots, axis=1).astype(jnp.int32)
    cell_flat = cell_order.reshape(-1)[tile_flat * CAP + piece_rank]
    tile_grid = tile_flat.reshape(NP // 2, CCDS, 2).transpose(1, 0, 2).reshape(CCDS, NP)
    cell_grid = cell_flat.reshape(NP // 2, CCDS, 2).transpose(1, 0, 2).reshape(CCDS, NP)
    scores = jax.random.randint(key_piece, (CCDS, NP), 0, 1 << 20).astype(jnp.int32) * NP + jnp.arange(NP, dtype=jnp.int32)[None, :]
    shuffle = jnp.argsort(scores, axis=1).astype(jnp.int32)
    return (jnp.take_along_axis(tile_grid, shuffle, axis=1).astype(jnp.int32), jnp.take_along_axis(cell_grid, shuffle, axis=1).astype(jnp.int32))


def draw_route_tile(key, part):
    return route_tables(key)[0]


def draw_route_cell(key, part):
    return route_tables(key)[1]


def place_ends(array, rng, smallest, largest):
    longest = array.shape.index(max(array.shape))
    spots = []
    for shift in (0, 1):
        where = [jax.random.randint(jax.random.fold_in(rng, axis), (), 0, length) for axis, length in enumerate(array.shape)]
        where[longest] = (where[longest] + shift) % array.shape[longest]
        spots.append(tuple(where))
    return array.at[spots[0]].set(smallest).at[spots[1]].set(largest)


def block_levels(key, extent, shards, least, high):
    loudness = 1.0
    for axis_at, shards_of in shards:
        steps = jax.random.uniform(jax.random.fold_in(jax.random.fold_in(key, 6), axis_at), (shards_of,), jnp.float32, least / len(shards), high / len(shards))
        loudness = loudness * jnp.repeat(jnp.exp(steps), extent[axis_at] // shards_of).reshape((-1,) + (1,) * (len(extent) - 1 - axis_at))
    return loudness


def gaussian(own_key, shape, scale, most, cuts=(), kind=jnp.bfloat16):
    array = scale * jax.random.normal(own_key, shape, jnp.float32)
    if cuts:
        array = array * block_levels(own_key, shape, cuts, -0.22, 0.18)
    return jnp.clip(array, -most, most).astype(kind)


def setup_inputs(seed: int = 0) -> dict:
    key_of = jax.random.split(jax.random.key(seed), 12)
    return {
        "exposure": gaussian(key_of[0], (CCDS, CROWS, W), 1.0, 6.0, ((0, 128), (1, 2)), jnp.float32),
        "row_shift": place_ends(jax.random.randint(key_of[1], (CCDS,), 0, HALO), jax.random.fold_in(key_of[1], 1), 0, HALO - 1).astype(jnp.int32),
        "row_fraction": jnp.clip(1.0 * jax.random.uniform(key_of[2], (CCDS, CROWS), jnp.float32) ** block_levels(key_of[2], (CCDS, CROWS), ((0, 128), (1, 2)), -0.2, 0.2), 0.0, 1.0).astype(jnp.bfloat16),
        "column_shift": place_ends(jax.random.randint(key_of[3], (CCDS,), 0, PW), jax.random.fold_in(key_of[3], 1), 0, PW - 1).astype(jnp.int32),
        "column_fraction": jnp.clip(1.0 * jax.random.uniform(key_of[4], (CCDS, W), jnp.float32) ** block_levels(key_of[4], (CCDS, W), ((0, 128),), -0.2, 0.2), 0.0, 1.0).astype(jnp.bfloat16),
        "piece_width": place_ends(jax.random.randint(key_of[5], (CCDS, NP), 1, PW + 1), jax.random.fold_in(key_of[5], 1), 1, PW).astype(jnp.int32),
        "route_tile": draw_route_tile(jax.random.fold_in(key_of[11], 71), 0),
        "route_cell": draw_route_cell(jax.random.fold_in(key_of[11], 71), 0),
        "template": gaussian(key_of[8], (NT, CROWS, CAP * PW), 1.0, 6.0, ((0, 128), (1, 2)), jnp.float32),
        "match_kernel": gaussian(key_of[9], (NT, KS, KS), (KS * KS) ** -0.5, 0.15625, ((0, 128),)),
        "detection_kernel": gaussian(key_of[10], (NT, DK, DK), (DK * DK) ** -0.5, 0.375, ((0, 128),)),
    }


def warp_columns(padded, column_offset, fraction):
    length = fraction.shape[-1]
    leftward = lax.dynamic_slice_in_dim(padded, column_offset, length, 1).astype(jnp.float32)
    rightward = lax.dynamic_slice_in_dim(padded, column_offset + 1, length, 1).astype(jnp.float32)
    weight = fraction.astype(jnp.float32)[None, :]
    return (1.0 - weight) * leftward + weight * rightward

def correlate(source, kernel):
    margin = kernel.shape[0] // 2
    output = lax.conv_general_dilated(source[None, None], kernel[None, None], (1, 1), [(margin, margin), (margin, margin)], precision=lax.Precision.HIGHEST)
    return output[0, 0]

def warp_exposure(frame_band, shift_rows, fraction_rows, shift_columns, fraction_columns):
    height = frame_band.shape[0]
    extended = jnp.concatenate([frame_band, jnp.zeros((HALO, frame_band.shape[1]), jnp.float32)], axis=0)
    upper_rows = lax.dynamic_slice_in_dim(extended, shift_rows, height, 0)
    lower_rows = lax.dynamic_slice_in_dim(extended, shift_rows + 1, height, 0)
    weight = fraction_rows.astype(jnp.float32)[:, None]
    warped_rows = ((1.0 - weight) * upper_rows + weight * lower_rows).astype(jnp.bfloat16)
    padded = jnp.pad(warped_rows, ((0, 0), (0, PW)))
    return warp_columns(padded, shift_columns, fraction_columns).astype(jnp.bfloat16)

def match_one(operands):
    return correlate(operands[0].astype(jnp.float32), operands[1].astype(jnp.float32))

def reference(exposure, row_shift, row_fraction, column_shift, column_fraction, piece_width, route_tile, route_cell, template, match_kernel, detection_kernel):
    warped = jax.vmap(warp_exposure)(exposure, row_shift, row_fraction, column_shift, column_fraction)
    lane_index = jnp.arange(PW, dtype=jnp.int32)
    keep_mask = lane_index[None, None, :] < piece_width[:, :, None]
    shaped = warped.reshape(CCDS, CROWS, NP, PW)
    shaped = jnp.where(keep_mask[:, None, :, :], shaped, jnp.zeros((), jnp.bfloat16))
    pieces = shaped.transpose(0, 2, 1, 3).reshape(CCDS * NP, CROWS, PW)
    target = (route_tile * CAP + route_cell).reshape(-1).astype(jnp.int32)
    placed = jnp.zeros((NT * CAP, CROWS, PW), jnp.bfloat16).at[target].set(pieces)
    science = placed.reshape(NT, CAP, CROWS, PW).transpose(0, 2, 1, 3).reshape(NT, CROWS, CAP * PW).astype(jnp.float32)
    cell_width = jnp.zeros((NT * CAP,), jnp.int32).at[target].set(piece_width.reshape(-1).astype(jnp.int32))
    live_mask = (lane_index[None, None, :] < cell_width.reshape(NT, CAP, 1)).reshape(NT, 1, CAP * PW)
    rounded = lax.optimization_barrier(template.astype(jnp.bfloat16))
    matched = lax.map(match_one, (rounded, match_kernel))
    difference = jnp.where(live_mask, science - matched, jnp.zeros((), jnp.float32))
    rounded_difference = lax.optimization_barrier(difference.astype(jnp.bfloat16))
    filtered = lax.map(match_one, (rounded_difference, detection_kernel))
    square_sum = jnp.sum(difference * difference)
    live_count = (CROWS * jnp.sum(cell_width)).astype(jnp.float32)
    noise_level = square_sum / live_count
    detect_weights = detection_kernel.astype(jnp.float32)
    kernel_norm = lax.optimization_barrier(jnp.sum(detect_weights * detect_weights, axis=(1, 2)))
    significance = filtered / jnp.sqrt(1.0 + noise_level * kernel_norm)[:, None, None]
    return (difference, significance, noise_level)
```

```python
import functools

import jax
import jax.numpy as jnp
from jax import lax
from jax.experimental import pallas as pl
from jax.experimental.pallas import tpu as pltpu
from jax.sharding import Mesh
from jax.sharding import PartitionSpec as P

PW = 128
HALO = 8
KS = 41
DK = 15
NZ, NX, NY = 8, 4, 4
GROUP = NZ * NY
NP = 16
CAP = 32
ROWS = 24
FR = ROWS // NZ
FL = PW // NY
MESH = pl.DeviceIdType.MESH
CCD = ("ccd_0", "ccd_1", "ccd_2")
F32, BF16, I32 = jnp.float32, jnp.bfloat16, jnp.int32


def lanes_of(shape):
    return lax.broadcasted_iota(I32, shape, len(shape) - 1)


def column_of(row, count):
    spread = jnp.broadcast_to(row, (count, count))
    pick = lax.broadcasted_iota(I32, (count, count), 0) == lanes_of((count, count))
    return jnp.sum(jnp.where(pick, spread, 0.0), axis=1, keepdims=True)


def down(x):
    rolled = pltpu.roll(x, 1, 0)
    return jnp.where(lax.broadcasted_iota(I32, x.shape, 0) == 0, 0.0, rolled)


def up(x):
    rolled = pltpu.roll(x, x.shape[0] - 1, 0)
    return jnp.where(lax.broadcasted_iota(I32, x.shape, 0) == x.shape[0] - 1, 0.0, rolled)


def build_bands(kernel_ref, extent, base_lo, base_hi, bands):
    depth = lax.broadcasted_iota(I32, (extent, 2 * PW), 0)
    place = lanes_of((extent, 2 * PW))
    picker = (lax.rem(depth + place, 2 * PW) == 0).astype(F32).astype(BF16)
    turned = jnp.dot(kernel_ref[...], picker, preferred_element_type=F32)
    for s in range(8):
        rolled = pltpu.roll(turned, s, 1) if s else turned
        base_lo[pl.ds(s, extent, stride=8), :] = rolled[:, :PW]
        base_hi[pl.ds(s, extent, stride=8), :] = rolled[:, PW:]
    bands[0:2 * PW, PW:] = jnp.zeros((2 * PW, PW), BF16)
    bands[extent * 2 * PW:(extent + 1) * 2 * PW, :PW] = jnp.zeros((2 * PW, PW), BF16)
    lane = lanes_of((8, PW))

    def step(a, carry):
        lo = base_lo[pl.ds(pl.multiple_of(a * 8, 8), 8), :]
        hi = base_hi[pl.ds(pl.multiple_of(a * 8, 8), 8), :]
        for pair in range(8):
            near, far = [], []
            for m in (2 * pair, 2 * pair + 1):
                shift = 8 * m
                rlo = pltpu.roll(lo, shift, 1) if shift else lo
                rhi = pltpu.roll(hi, shift, 1) if shift else hi
                near.append(jnp.where(lane >= shift, rlo, rhi))
                far.append(jnp.where(lane >= shift, rhi, rlo))
            for value, start in ((near, 16 * pair), (far, PW + 16 * pair)):
                block = jnp.concatenate(value, axis=0).astype(BF16)
                at = pl.multiple_of(a * 2 * PW + start, 16)
                bands[pl.ds(at, 16), 0:PW] = block
                after = pl.multiple_of((a + 1) * 2 * PW + start, 16)
                bands[pl.ds(after, 16), PW:2 * PW] = block
        return carry

    lax.fori_loop(0, extent, step, 0)


def build_windows(rows_ref, count, margin, windows):
    lane = lanes_of((CAP, PW))

    def step(h, carry):
        for parity in range(2):
            shifted = pltpu.roll(rows_ref[2 * h + parity].astype(F32), margin, 1)
            first = jnp.where(lane < margin, down(shifted), shifted)
            second = jnp.where(lane < margin, shifted, up(shifted))
            at = pl.ds(pl.multiple_of(h * CAP, CAP), CAP)
            windows[parity, at, 0:PW] = first.astype(BF16)
            windows[parity, at, PW:2 * PW] = second.astype(BF16)
        return carry

    lax.fori_loop(0, count // 2, step, 0)


def banded(windows, bands, extent, per_step, total):
    half = ROWS // 2 * CAP
    taps = (extent + 1) // 2

    def part(step):
        left = []
        for i in range(per_step):
            at = pl.ds(pl.multiple_of((step * per_step + i) * CAP, CAP), half)
            left += [windows[0, at, :], windows[1, at, :]]
        depth = per_step * 4 * PW
        right = bands[pl.ds(pl.multiple_of(step * depth, depth), depth), :]
        return jnp.dot(jnp.concatenate(left, axis=1), right, preferred_element_type=F32)

    total[...] = part(0)

    def step(i, carry):
        total[...] += part(i)
        return carry

    lax.fori_loop(1, taps // per_step, step, 0)


def kernel(
    exposure, template, row_shift, column_shift, row_fraction, column_fraction,
    piece_width, route_tile, route_cell, match_kernel, detection_kernel,
    difference, significance, noise,
    ext, hx, tf, tb, rfw, cfw, meta, msg, rcv, agb, acc, outg, grcv,
    base_lo, base_hi, bands, dbands, windows, dwindows, total, matched, diffs, db,
    arsrc, arcv, ar2src, arcv2, local, sends, recvs,
):
    z, x, y = (lax.axis_index(a) for a in CCD)
    c = lax.axis_index("row")
    me = z * NY + y

    def zpeer(dz, dy):
        pz = lax.rem(z + dz, NZ)
        py = lax.rem(y + dy, NY)
        return pz, py, {"ccd_0": pz, "ccd_2": py}

    def xpeer(dx, dc=0):
        return {"ccd_1": lax.rem(x + dx, NX), "row": lax.rem(c + dc, 2)}

    partner = {"row": 1 - c}
    near = [(dz, dy) for dz in range(NZ) for dy in range(NY) if dz or dy]
    across = [(dx, dc) for dx in range(NX) for dc in range(2) if dx or dc]

    def send(src, dst, stage, device, slot=None):
        pltpu.make_async_remote_copy(
            src_ref=src, dst_ref=dst, send_sem=sends.at[stage], recv_sem=recvs.at[stage if slot is None else slot],
            device_id=device, device_id_type=MESH,
        ).start()

    def arrived(ref, slot):
        pltpu.make_async_copy(ref, ref, recvs.at[slot]).wait()

    def sent(ref, stage):
        pltpu.make_async_copy(ref, ref, sends.at[stage]).wait()

    for p in range(NP):
        pltpu.make_async_copy(exposure.at[:, pl.ds(p * PW, PW)], ext.at[pl.ds(0, ROWS), p, :], local.at[0]).start()
    for q in range(CAP):
        pltpu.make_async_copy(template.at[:, pl.ds(q * PW, PW)], tf.at[:, q, :], local.at[1]).start()
    barrier = pltpu.get_barrier_semaphore()
    for dz, dy in near:
        pl.semaphore_signal(barrier, inc=1, device_id=zpeer(dz, dy)[2], device_id_type=MESH)
    for dx, dc in across:
        pl.semaphore_signal(barrier, inc=1, device_id=xpeer(dx, dc), device_id_type=MESH)

    fractions = row_fraction[...].astype(F32)
    for r in range(ROWS):
        rfw[r] = jnp.broadcast_to(fractions[:, r:r + 1], (1, PW))
    columns = column_fraction[...].astype(F32)
    for p in range(NP):
        cfw[p:p + 1, :] = columns[:, p * PW:(p + 1) * PW]
    lane16 = lanes_of((NP, PW))
    width16 = column_of(piece_width[...].astype(F32), NP)
    tile16 = column_of(route_tile[...].astype(F32), NP)
    cell16 = column_of(route_cell[...].astype(F32), NP)
    meta[...] = jnp.where(lane16 == 96, tile16, jnp.where(lane16 == 97, cell16, jnp.where(lane16 == 98, width16, 0.0)))
    build_bands(match_kernel, KS, base_lo, base_hi, bands)
    margin = KS // 2
    pltpu.make_async_copy(tf, tf, local.at[1]).wait()

    def round_template(r, carry):
        tb[margin + r] = tf[r].astype(BF16)
        return carry

    lax.fori_loop(0, ROWS, round_template, 0)

    def zero_template(r, carry):
        tb[c * (ROWS + margin) + r] = jnp.zeros((CAP, PW), BF16)
        return carry

    lax.fori_loop(0, margin, zero_template, 0)
    pltpu.make_async_copy(ext.at[pl.ds(0, ROWS)], ext.at[pl.ds(0, ROWS)], local.at[0]).wait()
    pl.semaphore_wait(barrier, len(near) + len(across))

    send(ext.at[pl.ds(0, HALO)], hx, 0, partner)
    send(tb.at[pl.ds(margin + (1 - c) * (ROWS - margin), margin)], tb.at[pl.ds(c * (ROWS + margin), margin)], 1, partner)
    arrived(hx, 0)
    keep = jnp.where(c == 0, 1.0, 0.0)
    for r in range(HALO):
        ext[ROWS + r] = hx[r] * keep

    t = row_shift[0]
    s = column_shift[0]
    left_turn = lax.rem(PW - s, PW)
    right_turn = PW - 1 - s
    weight = cfw[...]
    inside = lane16.astype(F32) < width16
    head = meta[...]

    def fragments(pz):
        rows = []
        for j in range(FR):
            r = pz * FR + j
            w = rfw[r]
            mixed = ((1.0 - w) * ext[r + t] + w * ext[r + t + 1]).astype(BF16).astype(F32)
            leftward = pltpu.roll(mixed, left_turn, 1)
            leftward = jnp.where(lane16 < PW - s, leftward, up(leftward))
            rightward = pltpu.roll(mixed, right_turn, 1)
            rightward = jnp.where(lane16 < PW - 1 - s, rightward, up(rightward))
            warped = (1.0 - weight) * leftward + weight * rightward
            rows.append(jnp.where(inside, warped, 0.0))
        out = []
        for py in range(NY):
            value = head
            for j in range(FR):
                turn = (FL * (j - py)) % PW
                moved = pltpu.roll(rows[j], turn, 1) if turn else rows[j]
                value = jnp.where((lane16 >= FL * j) & (lane16 < FL * (j + 1)), moved, value)
            out.append(value.astype(BF16))
        return out

    def spread(dz, carry):
        pz = lax.rem(z + dz, NZ)
        for py, value in enumerate(fragments(pz)):
            msg[pz * NY + py] = value
        for dy in range(NY):
            _, py, device = zpeer(dz, dy)
            send(msg.at[pz * NY + py], rcv.at[me], 2, device)
        return carry

    lax.fori_loop(1, NZ, spread, 0)
    for py, value in enumerate(fragments(z)):
        msg[z * NY + py] = value
    for dy in range(1, NY):
        _, py, device = zpeer(0, dy)
        send(msg.at[z * NY + py], rcv.at[me], 2, device)
    rcv[me] = msg[me]

    arrived(hx_template(tb, margin, c), 1)
    build_windows(tb, ROWS + 2 * margin, margin, windows)
    banded(windows, bands, KS, 3, total)

    def unpair(q, carry):
        at = pl.ds(pl.multiple_of(q * CAP, CAP), CAP)
        matched[2 * q] = total[at, 0:PW]
        matched[2 * q + 1] = total[at, PW:2 * PW]
        return carry

    lax.fori_loop(0, ROWS // 2, unpair, 0)
    build_bands(detection_kernel, DK, base_lo, base_hi, dbands)
    arrived(rcv.at[pl.ds(0, GROUP - 1)], 2)

    for dx in (1, 3, 2):
        send(rcv, agb.at[dx - 1], 3, xpeer(dx), slot=8 + dx)

    def codes(block):
        picks = (lanes_of((8, PW)) == lax.broadcasted_iota(I32, (8, PW), 0) + 96).astype(F32).astype(BF16)
        rows = lax.dot_general(picks, block, (((1,), (1,)), ((), ())), preferred_element_type=F32)
        tile = rows[0:1, :].astype(I32)
        cell = rows[1:2, :].astype(I32)
        tz, tx, ty = tile // (NX * NY), (tile // NY) % NX, tile % NY
        return jnp.where(tx == x, (tz * NY + ty) * CAP + cell, -1)

    chunk = NY * CAP
    chunk_rows = lax.broadcasted_iota(I32, (chunk, GROUP * NP), 0)

    def chosen(code, block, pz):
        hot = (chunk_rows == code - pz * chunk).astype(F32).astype(BF16)
        return jnp.dot(hot, block, preferred_element_type=F32)

    def flat(ref):
        return ref[...].reshape(GROUP * NP, PW)

    def add_block(block, first):
        code = codes(block)

        def step(pz, carry):
            at = pl.ds(pl.multiple_of(pz * chunk, chunk), chunk)
            value = chosen(code, block, pz)
            acc[at, :] = value if first else acc[at, :] + value
            return carry

        lax.fori_loop(0, NZ, step, 0)

    add_block(flat(rcv), True)
    arrived(agb.at[0], 9)
    add_block(flat(agb.at[0]), False)
    arrived(agb.at[2], 11)
    add_block(flat(agb.at[2]), False)
    arrived(agb.at[1], 10)
    block = flat(agb.at[1])
    code = codes(block)

    def finish(pz):
        at = pl.ds(pl.multiple_of(pz * chunk, chunk), chunk)
        value = (acc[at, :] + chosen(code, block, pz)).astype(BF16)
        for py in range(NY):
            outg[pz * NY + py] = value[py * CAP:(py + 1) * CAP]

    def deliver(dz, carry):
        pz = lax.rem(z + dz, NZ)
        finish(pz)
        for dy in range(NY):
            _, py, device = zpeer(dz, dy)
            send(outg.at[pz * NY + py], grcv.at[me], 4, device)
        return carry

    lax.fori_loop(1, NZ, deliver, 0)
    finish(z)
    for dy in range(1, NY):
        _, py, device = zpeer(0, dy)
        send(outg.at[z * NY + py], grcv.at[me], 4, device)
    grcv[me] = outg[me]
    sent(rcv.at[pl.ds(0, GROUP - 1)], 2)
    sent(agb, 3)
    sent(hx, 0)
    sent(tb.at[pl.ds(0, margin)], 1)

    dmargin = DK // 2

    def zero_difference(r, carry):
        db[c * (ROWS + dmargin) + r] = jnp.zeros((CAP, PW), BF16)
        return carry

    lax.fori_loop(0, dmargin, zero_difference, 0)
    arrived(grcv.at[pl.ds(0, GROUP - 1)], 4)

    lane32 = lanes_of((CAP, PW))
    own = grcv[me].astype(F32)
    width32 = jnp.sum(jnp.where(lane32 == 98, own, 0.0), axis=1, keepdims=True)
    live = lane32.astype(F32) < width32

    def subtract(pz, squares):
        parts = [grcv[pz * NY + py].astype(F32) for py in range(NY)]
        for j in range(FR):
            science = None
            for py in range(NY):
                turn = (FL * (py - j)) % PW
                moved = pltpu.roll(parts[py], turn, 1) if turn else parts[py]
                science = moved if science is None else jnp.where(lane32 >= FL * py, moved, science)
            r = pz * FR + j
            value = jnp.where(live, science - matched[r], 0.0)
            diffs[r] = value
            db[dmargin + r] = value.astype(BF16)
            squares = squares + value * value
        return squares

    squares = lax.fori_loop(0, NZ, subtract, jnp.zeros((CAP, PW), F32))
    square_sum = jnp.sum(jnp.sum(squares, axis=1, keepdims=True), axis=0, keepdims=True)
    live_count = ROWS * jnp.sum(width32, axis=0, keepdims=True)
    lane1 = lanes_of((1, PW))
    arsrc[...] = jnp.where(lane1 == 0, square_sum, jnp.where(lane1 == 1, live_count, 0.0))
    for dz, dy in near:
        send(arsrc, arcv.at[me], 5, zpeer(dz, dy)[2])
    arcv[me] = arsrc[...]
    send(db.at[pl.ds(dmargin + (1 - c) * (ROWS - dmargin), dmargin)], db.at[pl.ds(c * (ROWS + dmargin), dmargin)], 6, partner)
    for q in range(CAP):
        pltpu.make_async_copy(diffs.at[:, q, :], difference.at[:, pl.ds(q * PW, PW)], local.at[2]).start()
    arrived(hx_template(db, dmargin, c), 6)

    build_windows(db, ROWS + 2 * dmargin, dmargin, dwindows)
    banded(dwindows, dbands, DK, 2, total)
    arrived(arcv.at[pl.ds(0, GROUP - 1)], 5)
    ar2src[...] = jnp.sum(arcv[...], axis=0)
    for dx, dc in across:
        send(ar2src, arcv2.at[x * 2 + c], 7, xpeer(dx, dc))
    arcv2[x * 2 + c] = ar2src[...]
    arrived(arcv2.at[pl.ds(0, 7)], 7)
    sums = jnp.sum(arcv2[...], axis=0)
    whole_square = jnp.sum(jnp.where(lane1 == 0, sums, 0.0), axis=1, keepdims=True)
    whole_count = jnp.sum(jnp.where(lane1 == 1, sums, 0.0), axis=1, keepdims=True)
    level = whole_square / whole_count
    taps = detection_kernel[...].astype(F32)
    norm = jnp.sum(jnp.sum(taps * taps, axis=1, keepdims=True), axis=0, keepdims=True)
    scale = jnp.broadcast_to(1.0 / jnp.sqrt(1.0 + level * norm), (CAP, PW))
    noise[...] = jnp.broadcast_to(level, (1, PW))

    def rescale(q, carry):
        at = pl.ds(pl.multiple_of(q * CAP, CAP), CAP)
        tf[2 * q] = total[at, 0:PW] * scale
        tf[2 * q + 1] = total[at, PW:2 * PW] * scale
        return carry

    lax.fori_loop(0, ROWS // 2, rescale, 0)
    for q in range(CAP):
        pltpu.make_async_copy(tf.at[:, q, :], significance.at[:, pl.ds(q * PW, PW)], local.at[3]).start()
    sent(grcv.at[pl.ds(0, GROUP - 1)], 4)
    sent(arcv.at[pl.ds(0, GROUP - 1)], 5)
    sent(db.at[pl.ds(0, dmargin)], 6)
    sent(arcv2.at[pl.ds(0, 7)], 7)
    pltpu.make_async_copy(diffs, diffs, local.at[2]).wait()
    pltpu.make_async_copy(tf, tf, local.at[3]).wait()


def hx_template(ref, margin, c):
    return ref.at[pl.ds((1 - c) * (ROWS + margin), margin)]


def on_device(
    exposure, row_shift, row_fraction, column_shift, column_fraction, piece_width,
    route_tile, route_cell, template, match_kernel, detection_kernel,
):
    vmem = pl.BlockSpec(memory_space=pltpu.VMEM)
    smem = pl.BlockSpec(memory_space=pltpu.SMEM)
    far = pl.BlockSpec(memory_space=pl.ANY)
    wide = template.shape[2]
    margin, dmargin = KS // 2, DK // 2
    difference, significance, noise = pl.pallas_call(
        kernel,
        out_shape=(
            jax.ShapeDtypeStruct((ROWS, wide), F32),
            jax.ShapeDtypeStruct((ROWS, wide), F32),
            jax.ShapeDtypeStruct((1, PW), F32),
        ),
        in_specs=[far, far, smem, smem] + [vmem] * 7,
        out_specs=(far, far, vmem),
        scratch_shapes=[
            pltpu.VMEM((ROWS + HALO, NP, PW), F32),
            pltpu.VMEM((HALO, NP, PW), F32),
            pltpu.VMEM((ROWS, CAP, PW), F32),
            pltpu.VMEM((ROWS + 2 * margin, CAP, PW), BF16),
            pltpu.VMEM((ROWS, 1, PW), F32),
            pltpu.VMEM((NP, PW), F32),
            pltpu.VMEM((NP, PW), F32),
            pltpu.VMEM((GROUP, NP, PW), BF16),
            pltpu.VMEM((GROUP, NP, PW), BF16),
            pltpu.VMEM((NX - 1, GROUP, NP, PW), BF16),
            pltpu.VMEM((GROUP * CAP, PW), F32),
            pltpu.VMEM((GROUP, CAP, PW), BF16),
            pltpu.VMEM((GROUP, CAP, PW), BF16),
            pltpu.VMEM((48 * 8, PW), F32),
            pltpu.VMEM((48 * 8, PW), F32),
            pltpu.VMEM(((KS + 1) * 2 * PW, 2 * PW), BF16),
            pltpu.VMEM(((DK + 1) * 2 * PW, 2 * PW), BF16),
            pltpu.VMEM((2, (ROWS // 2 + margin) * CAP, 2 * PW), BF16),
            pltpu.VMEM((2, (ROWS // 2 + dmargin) * CAP, 2 * PW), BF16),
            pltpu.VMEM((ROWS // 2 * CAP, 2 * PW), F32),
            pltpu.VMEM((ROWS, CAP, PW), F32),
            pltpu.VMEM((ROWS, CAP, PW), F32),
            pltpu.VMEM((ROWS + 2 * dmargin, CAP, PW), BF16),
            pltpu.VMEM((1, PW), F32),
            pltpu.VMEM((GROUP, 1, PW), F32),
            pltpu.VMEM((1, PW), F32),
            pltpu.VMEM((8, 1, PW), F32),
            pltpu.SemaphoreType.DMA((4,)),
            pltpu.SemaphoreType.DMA((8,)),
            pltpu.SemaphoreType.DMA((12,)),
        ],
        compiler_params=pltpu.CompilerParams(collective_id=0, has_side_effects=True, vmem_limit_bytes=60 * 1024 * 1024),
        name="warp_match_detect",
    )(
        exposure[0], template[0], row_shift, column_shift, row_fraction, column_fraction,
        piece_width, route_tile, route_cell, match_kernel[0], detection_kernel[0],
    )
    return difference[None], significance[None], noise[0, 0]


def solution(mesh):
    finer = Mesh(
        mesh.devices.reshape(NZ, NX, NY, mesh.shape["row"]), ("ccd_0", "ccd_1", "ccd_2", "row")
    )
    placed = (
        P(CCD, "row", None),
        P(CCD),
        P(CCD, "row"),
        P(CCD),
        P(CCD, None),
        P(CCD, None),
        P(CCD, None),
        P(CCD, None),
        P(CCD, "row", None),
        P(CCD, None, None),
        P(CCD, None, None),
    )
    return jax.shard_map(
        on_device,
        mesh=finer,
        in_specs=placed,
        out_specs=(P(CCD, "row", None), P(CCD, "row", None), P()),
        check_vma=False,
    )
```

```python
import functools

import jax
import jax.numpy as jnp
from jax import lax
from jax.experimental import pallas as pl
from jax.experimental.pallas import tpu as pltpu
from jax.sharding import Mesh
from jax.sharding import PartitionSpec as P

PW = 128
HALO = 8
KS = 41
DK = 15
NZ, NX, NY = 8, 4, 4
GROUP = NZ * NY
NP = 16
CAP = 32
ROWS = 24
FR = ROWS // NZ
FL = PW // NY
EARLY = 18
MESH = pl.DeviceIdType.MESH
CCD = ("ccd_0", "ccd_1", "ccd_2")
F32, BF16, I32 = jnp.float32, jnp.bfloat16, jnp.int32


def lanes_of(shape):
    return lax.broadcasted_iota(I32, shape, len(shape) - 1)


def column_of(row, count):
    spread = jnp.broadcast_to(row, (count, count))
    pick = lax.broadcasted_iota(I32, (count, count), 0) == lanes_of((count, count))
    return jnp.sum(jnp.where(pick, spread, 0.0), axis=1, keepdims=True)


def down(x):
    rolled = pltpu.roll(x, 1, 0)
    return jnp.where(lax.broadcasted_iota(I32, x.shape, 0) == 0, 0.0, rolled)


def up(x):
    rolled = pltpu.roll(x, x.shape[0] - 1, 0)
    return jnp.where(lax.broadcasted_iota(I32, x.shape, 0) == x.shape[0] - 1, 0.0, rolled)


def band_bases(kernel_ref, extent, base_lo, base_hi, bands):
    depth = lax.broadcasted_iota(I32, (extent, 2 * PW), 0)
    place = lanes_of((extent, 2 * PW))
    picker = (lax.rem(depth + place, 2 * PW) == 0).astype(F32).astype(BF16)
    turned = jnp.dot(kernel_ref[...], picker, preferred_element_type=F32)
    for s in range(8):
        rolled = pltpu.roll(turned, s, 1) if s else turned
        base_lo[pl.ds(s, extent, stride=8), :] = rolled[:, :PW]
        base_hi[pl.ds(s, extent, stride=8), :] = rolled[:, PW:]
    bands[0:2 * PW, PW:] = jnp.zeros((2 * PW, PW), BF16)
    bands[extent * 2 * PW:(extent + 1) * 2 * PW, :PW] = jnp.zeros((2 * PW, PW), BF16)


def build_bands(base_lo, base_hi, bands, first, last):
    lane = lanes_of((8, PW))

    def step(a, carry):
        lo = base_lo[pl.ds(pl.multiple_of(a * 8, 8), 8), :]
        hi = base_hi[pl.ds(pl.multiple_of(a * 8, 8), 8), :]
        for pair in range(8):
            near, far = [], []
            for m in (2 * pair, 2 * pair + 1):
                shift = 8 * m
                rlo = pltpu.roll(lo, shift, 1) if shift else lo
                rhi = pltpu.roll(hi, shift, 1) if shift else hi
                near.append(jnp.where(lane >= shift, rlo, rhi))
                far.append(jnp.where(lane >= shift, rhi, rlo))
            for value, start in ((near, 16 * pair), (far, PW + 16 * pair)):
                block = jnp.concatenate(value, axis=0).astype(BF16)
                at = pl.multiple_of(a * 2 * PW + start, 16)
                bands[pl.ds(at, 16), 0:PW] = block
                after = pl.multiple_of((a + 1) * 2 * PW + start, 16)
                bands[pl.ds(after, 16), PW:2 * PW] = block
        return carry

    lax.fori_loop(first, last, step, 0)


def build_windows(rows_ref, start, count, margin, windows, unroll):
    lane = lanes_of((CAP, PW))

    def step(i, carry):
        r = start + i
        shifted = pltpu.roll(rows_ref[r].astype(F32), margin, 1)
        first = jnp.where(lane < margin, down(shifted), shifted)
        second = jnp.where(lane < margin, shifted, up(shifted))
        at = pl.ds(pl.multiple_of(r // 2 * CAP, CAP), CAP)
        windows[r % 2, at, 0:PW] = first.astype(BF16)
        windows[r % 2, at, PW:2 * PW] = second.astype(BF16)
        return carry

    lax.fori_loop(0, count, step, 0, unroll=unroll)


def clear_windows(start, count, windows):
    def step(i, carry):
        r = start + i
        at = pl.ds(pl.multiple_of(r // 2 * CAP, CAP), CAP)
        windows[r % 2, at, :] = jnp.zeros((CAP, 2 * PW), BF16)
        return carry

    lax.fori_loop(0, count, step, 0)


def near_first(i):
    half = (i + 1) // 2
    return lax.rem(half * (2 * (i % 2) - 1) + NZ, NZ)


def far_first(i):
    half = (i + 1) // 2
    return lax.rem(NZ // 2 + half * (1 - 2 * (i % 2)) + NZ, NZ)


def banded(windows, bands, per_step, first, last, total):
    half = ROWS // 2 * CAP

    def part(step):
        left = []
        for i in range(per_step):
            at = pl.ds(pl.multiple_of((step * per_step + i) * CAP, CAP), half)
            left += [windows[0, at, :], windows[1, at, :]]
        depth = per_step * 4 * PW
        right = bands[pl.ds(pl.multiple_of(step * depth, depth), depth), :]
        return jnp.dot(jnp.concatenate(left, axis=1), right, preferred_element_type=F32)

    if first == 0:
        total[...] = part(0)

    def step(i, carry):
        total[...] += part(i)
        return carry

    lax.fori_loop(max(first, 1), last, step, 0)


def kernel(
    exposure, template, *rest):
    small, rest = rest[:9], rest[9:]
    (difference, significance, noise, scale,
    ext, hx, tf, tb, rfw, cfw, meta, msg, rcv, agb, acc, outg, grcv, held, mfr, mrc,
    base_lo, base_hi, bands, dbands, windows, dwindows, total, matched, diffs, db,
    arsrc, arcv, ar2src, arcv2, local, sends, recvs,
    row_shift, column_shift, row_fraction, column_fraction,
    piece_width, route_tile, route_cell, match_kernel, detection_kernel) = rest
    z, x, y = (lax.axis_index(a) for a in CCD)
    c = lax.axis_index("row")
    me = z * NY + y

    def zpeer(dz, dy):
        pz = lax.rem(z + dz, NZ)
        py = lax.rem(y + dy, NY)
        return pz, py, {"ccd_0": pz, "ccd_2": py}

    def xpeer(dx, dc=0):
        return {"ccd_1": lax.rem(x + dx, NX), "row": lax.rem(c + dc, 2)}

    partner = {"row": 1 - c}
    near = [(dz, dy) for dz in range(NZ) for dy in range(NY) if dz or dy]
    across = [(dx, dc) for dx in range(NX) for dc in range(2) if dx or dc]

    def send(src, dst, stage, device, slot=None):
        pltpu.make_async_remote_copy(
            src_ref=src, dst_ref=dst, send_sem=sends.at[stage], recv_sem=recvs.at[stage if slot is None else slot],
            device_id=device, device_id_type=MESH,
        ).start()

    def arrived(ref, slot):
        pltpu.make_async_copy(ref, ref, recvs.at[slot]).wait()

    def sent(ref, stage):
        pltpu.make_async_copy(ref, ref, sends.at[stage]).wait()

    barrier = pltpu.get_barrier_semaphore()
    for dz, dy in near:
        pl.semaphore_signal(barrier, inc=1, device_id=zpeer(dz, dy)[2], device_id_type=MESH)
    for dx, dc in across:
        pl.semaphore_signal(barrier, inc=1, device_id=xpeer(dx, dc), device_id_type=MESH)
    held_small = (
        row_shift, column_shift, row_fraction, column_fraction,
        piece_width, route_tile, route_cell, match_kernel, detection_kernel,
    )
    loads = [pltpu.make_async_copy(src, dst, local.at[4 + i]) for i, (src, dst) in enumerate(zip(small, held_small))]
    for load in loads:
        load.start()
    for q in range(CAP):
        pltpu.make_async_copy(template.at[:, pl.ds(q * PW, PW)], tf.at[:, q, :], local.at[1]).start()
    for p in range(NP):
        pltpu.make_async_copy(exposure.at[:, pl.ds(p * PW, PW)], ext.at[pl.ds(0, ROWS), p, :], local.at[0]).start()
    for load in loads:
        load.wait()

    fractions = row_fraction[...].astype(F32)
    for r in range(ROWS):
        rfw[r] = jnp.broadcast_to(fractions[:, r:r + 1], (1, PW))
    columns = column_fraction[...].astype(F32)
    for p in range(NP):
        cfw[p:p + 1, :] = columns[:, p * PW:(p + 1) * PW]
    lane16 = lanes_of((NP, PW))
    width16 = column_of(piece_width[...].astype(F32), NP)
    tile16 = column_of(route_tile[...].astype(F32), NP)
    cell16 = column_of(route_cell[...].astype(F32), NP)
    meta[...] = jnp.where(lane16 == 96, tile16, jnp.where(lane16 == 97, cell16, jnp.where(lane16 == 98, width16, 0.0)))
    margin, dmargin = KS // 2, DK // 2
    pltpu.make_async_copy(tf, tf, local.at[1]).wait()

    def round_template(r, carry):
        tb[margin + r] = tf[r].astype(BF16)
        return carry

    lax.fori_loop(0, ROWS, round_template, 0, unroll=4)
    band_bases(match_kernel, KS, base_lo, base_hi, bands)
    build_bands(base_lo, base_hi, bands, 0, EARLY)
    clear_windows(c * (ROWS + margin), margin, windows)
    clear_windows(c * (ROWS + dmargin), dmargin, dwindows)
    pltpu.make_async_copy(ext.at[pl.ds(0, ROWS)], ext.at[pl.ds(0, ROWS)], local.at[0]).wait()
    pl.semaphore_wait(barrier, len(near) + len(across))

    send(ext.at[pl.ds(0, HALO)], hx, 0, partner)
    send(tb.at[pl.ds(margin + (1 - c) * (ROWS - margin), margin)], tb.at[pl.ds(c * (ROWS + margin), margin)], 1, partner)
    build_windows(tb, margin, ROWS, margin, windows, 4)
    arrived(hx, 0)
    keep = jnp.where(c == 0, 1.0, 0.0)
    for r in range(HALO):
        ext[ROWS + r] = hx[r] * keep

    t = row_shift[0]
    s = column_shift[0]
    left_turn = lax.rem(PW - s, PW)
    right_turn = PW - 1 - s
    weight = cfw[...]
    inside = lane16.astype(F32) < width16
    head = meta[...]

    def fragments(pz):
        rows = []
        for j in range(FR):
            r = pz * FR + j
            w = rfw[r]
            mixed = ((1.0 - w) * ext[r + t] + w * ext[r + t + 1]).astype(BF16).astype(F32)
            leftward = pltpu.roll(mixed, left_turn, 1)
            leftward = jnp.where(lane16 < PW - s, leftward, up(leftward))
            rightward = pltpu.roll(mixed, right_turn, 1)
            rightward = jnp.where(lane16 < PW - 1 - s, rightward, up(rightward))
            warped = (1.0 - weight) * leftward + weight * rightward
            rows.append(jnp.where(inside, warped, 0.0))
        out = []
        for py in range(NY):
            value = head
            for j in range(FR):
                turn = (FL * (j - py)) % PW
                moved = pltpu.roll(rows[j], turn, 1) if turn else rows[j]
                value = jnp.where((lane16 >= FL * j) & (lane16 < FL * (j + 1)), moved, value)
            out.append(value.astype(BF16))
        return out

    def spread(slot):
        def step(i, carry):
            dz = near_first(i)
            pz = lax.rem(z + dz, NZ)
            for py, value in enumerate(fragments(pz)):
                msg[pz * NY + py] = value
            for dy in range(NY):
                _, py, device = zpeer(dz, dy)
                send(msg.at[pz * NY + py], rcv.at[me], 2, device, slot)
            return carry

        return step

    for py, value in enumerate(fragments(z)):
        msg[z * NY + py] = value
    for dy in range(1, NY):
        _, py, device = zpeer(0, dy)
        send(msg.at[z * NY + py], rcv.at[me], 2, device, 2)
    lax.fori_loop(1, 3, spread(2), 0)
    lax.fori_loop(3, 5, spread(3), 0)
    lax.fori_loop(5, 8, spread(4), 0)
    rcv[me] = msg[me]

    def forward(slot, distances, count):
        arrived(rcv.at[pl.ds(0, count)], slot)
        for dz in distances:
            at = pl.ds(lax.rem(z + dz, NZ) * NY, NY)
            for dx in (2, 1, 3):
                send(rcv.at[at], agb.at[dx - 1, at], 3, xpeer(dx), slot=9 + dx)

    arrived(other_rows(tb, margin, c), 1)
    build_windows(tb, (1 - c) * (ROWS + margin), margin, margin, windows, 4)
    build_bands(base_lo, base_hi, bands, EARLY, KS)
    forward(2, (0, 1, 7), 11)
    banded(windows, bands, 3, 0, 3, total)
    forward(3, (2, 6), 8)
    banded(windows, bands, 3, 3, 7, total)
    forward(4, (3, 5, 4), 12)

    def unpair(q, carry):
        at = pl.ds(pl.multiple_of(q * CAP, CAP), CAP)
        matched[2 * q] = total[at, 0:PW]
        matched[2 * q + 1] = total[at, PW:2 * PW]
        return carry

    lax.fori_loop(0, ROWS // 2, unpair, 0, unroll=2)
    lane24 = lanes_of((ROWS, PW))

    def split(pz):
        for py in range(NY):
            value, last = None, []
            for j in range(FR):
                turn = (FL * (j - py)) % PW
                row = matched[pz * FR + j]
                moved = pltpu.roll(row[:ROWS], turn, 1) if turn else row[:ROWS]
                value = moved if value is None else jnp.where(lane24 >= FL * j, moved, value)
                turn = (FL * (FR - py)) % PW
                last.append(pltpu.roll(row[ROWS:], turn, 1) if turn else row[ROWS:])
            value = jnp.where(lane24 >= FR * FL, jnp.concatenate(last, axis=0), value)
            mfr[pz * NY + py] = value.astype(BF16)

    def follow(i, carry):
        dz = far_first(i)
        pz = lax.rem(z + dz, NZ)
        split(pz)
        for dy in range(NY):
            _, py, device = zpeer(dz, dy)
            send(mfr.at[pz * NY + py], mrc.at[me], 4, device, 5)
        return carry

    lax.fori_loop(0, NZ - 1, follow, 0)
    split(z)
    for dy in range(1, NY):
        _, py, device = zpeer(0, dy)
        send(mfr.at[z * NY + py], mrc.at[me], 4, device, 5)
    mrc[me] = mfr[me]

    def codes(block):
        picks = (lanes_of((8, PW)) == lax.broadcasted_iota(I32, (8, PW), 0) + 96).astype(F32).astype(BF16)
        rows = lax.dot_general(picks, block, (((1,), (1,)), ((), ())), preferred_element_type=F32)
        tile = rows[0:1, :].astype(I32)
        cell = rows[1:2, :].astype(I32)
        tz, tx, ty = tile // (NX * NY), (tile // NY) % NX, tile % NY
        return jnp.where(tx == x, (tz * NY + ty) * CAP + cell, -1)

    chunk = NY * CAP
    chunk_rows = lax.broadcasted_iota(I32, (chunk, GROUP * NP), 0)

    def chosen(code, block, pz):
        hot = (chunk_rows == code - pz * chunk).astype(F32).astype(BF16)
        return jnp.dot(hot, block, preferred_element_type=F32)

    def flat(ref):
        return ref[...].reshape(GROUP * NP, PW)

    def add_block(block, first):
        code = codes(block)

        def step(pz, carry):
            at = pl.ds(pl.multiple_of(pz * chunk, chunk), chunk)
            value = chosen(code, block, pz)
            acc[at, :] = value if first else acc[at, :] + value
            return carry

        lax.fori_loop(0, NZ, step, 0, unroll=8)

    add_block(flat(rcv), True)
    arrived(agb.at[2], 12)
    add_block(flat(agb.at[2]), False)
    arrived(agb.at[0], 10)
    add_block(flat(agb.at[0]), False)
    arrived(agb.at[1], 11)
    block = flat(agb.at[1])
    code = codes(block)

    lane8 = lanes_of((8, PW))

    def finish(pz):
        at = pl.ds(pl.multiple_of(pz * chunk, chunk), chunk)
        value = acc[at, :] + chosen(code, block, pz)
        acc[at, :] = value
        for py in range(NY):
            tile = value[py * CAP:(py + 1) * CAP]
            rows = []
            for j in range(FR):
                turn = (FL * (FR - j)) % PW
                rows.append(jnp.where(lane8 >= FR * FL, pltpu.roll(tile[ROWS:], turn, 1), tile[8 * j:8 * j + 8]))
            outg[pz * NY + py] = jnp.concatenate(rows, axis=0).astype(BF16)
        return value

    def deliver(i, carry):
        dz = far_first(i)
        pz = lax.rem(z + dz, NZ)
        finish(pz)
        for dy in range(NY):
            _, py, device = zpeer(dz, dy)
            send(outg.at[pz * NY + py], grcv.at[me], 5, device, 6)
        return carry

    lax.fori_loop(0, NZ - 1, deliver, 0, unroll=7)
    held[...] = finish(z)
    for dy in range(1, NY):
        _, py, device = zpeer(0, dy)
        send(outg.at[z * NY + py], grcv.at[me], 5, device, 6)
    grcv[me] = outg[me]

    lane32 = lanes_of((CAP, PW))
    own = held[pl.ds(pl.multiple_of(y * CAP, CAP), CAP), :]
    width32 = jnp.sum(jnp.where(lane32 == 98, own, 0.0), axis=1, keepdims=True)
    live = lane32.astype(F32) < width32
    live_count = ROWS * jnp.sum(width32, axis=0, keepdims=True)
    place = (lax.rem(lane24, FL) + FL * y).astype(F32)
    arrived(mrc.at[pl.ds(0, GROUP - 1)], 5)

    def square(k, squares):
        value = acc[pl.ds(pl.multiple_of(k * CAP, CAP), CAP), :]
        width = jnp.sum(jnp.where(lane32 == 98, value, 0.0), axis=1, keepdims=True)
        last = jnp.concatenate([width[ROWS:]] * FR, axis=0)
        width = jnp.where(lane24 < FR * FL, width[:ROWS], last)
        value = jnp.where(place < width, outg[k].astype(F32) - mrc[k].astype(F32), 0.0)
        return squares + value * value

    squares = lax.fori_loop(0, GROUP, square, jnp.zeros((ROWS, PW), F32), unroll=4)
    square_sum = jnp.sum(jnp.sum(squares, axis=1, keepdims=True), axis=0, keepdims=True)
    lane1 = lanes_of((1, PW))
    arsrc[...] = jnp.where(lane1 == 0, square_sum, jnp.where(lane1 == 1, live_count, 0.0))
    for dz, dy in near:
        send(arsrc, arcv.at[me], 6, zpeer(dz, dy)[2], 7)
    arcv[me] = arsrc[...]
    band_bases(detection_kernel, DK, base_lo, base_hi, dbands)
    build_bands(base_lo, base_hi, dbands, 0, DK)
    sent(rcv.at[pl.ds(0, GROUP - 1)], 2)
    sent(agb, 3)
    sent(hx, 0)
    sent(tb.at[pl.ds(0, margin)], 1)
    sent(mrc.at[pl.ds(0, GROUP - 1)], 4)
    arrived(grcv.at[pl.ds(0, GROUP - 1)], 6)

    def subtract(pz, carry):
        parts = [grcv[pz * NY + py].astype(F32) for py in range(NY)]
        for j in range(FR):
            science = None
            for py in range(NY):
                turn = (FL * (py - j)) % PW
                moved = pltpu.roll(parts[py], turn, 1) if turn else parts[py]
                turn = (FL * (py - FR)) % PW
                rest = parts[py][8 * j:8 * j + 8]
                rest = pltpu.roll(rest, turn, 1) if turn else rest
                moved = jnp.concatenate([moved, rest], axis=0)
                science = moved if science is None else jnp.where(lane32 >= FL * py, moved, science)
            r = pz * FR + j
            value = jnp.where(live, science - matched[r], 0.0)
            diffs[r] = value
            db[dmargin + r] = value.astype(BF16)
        return carry

    lax.fori_loop(0, NZ, subtract, 0)
    send(db.at[pl.ds(dmargin + (1 - c) * (ROWS - dmargin), dmargin)], db.at[pl.ds(c * (ROWS + dmargin), dmargin)], 8, partner, 9)
    for q in range(CAP):
        pltpu.make_async_copy(diffs.at[:, q, :], difference.at[:, pl.ds(q * PW, PW)], local.at[2]).start()
    build_windows(db, dmargin, ROWS, dmargin, dwindows, 4)
    arrived(arcv.at[pl.ds(0, GROUP - 1)], 7)
    ar2src[...] = jnp.sum(arcv[...], axis=0)
    for dx, dc in across:
        send(ar2src, arcv2.at[x * 2 + c], 7, xpeer(dx, dc), 8)
    arcv2[x * 2 + c] = ar2src[...]

    arrived(other_rows(db, dmargin, c), 9)
    build_windows(db, (1 - c) * (ROWS + dmargin), dmargin, dmargin, dwindows, 7)
    banded(dwindows, dbands, 2, 0, (DK + 1) // 4, total)

    def unpair_filtered(q, carry):
        at = pl.ds(pl.multiple_of(q * CAP, CAP), CAP)
        tf[2 * q] = total[at, 0:PW]
        tf[2 * q + 1] = total[at, PW:2 * PW]
        return carry

    lax.fori_loop(0, ROWS // 2, unpair_filtered, 0, unroll=2)
    for q in range(CAP):
        pltpu.make_async_copy(tf.at[:, q, :], significance.at[:, pl.ds(q * PW, PW)], local.at[3]).start()
    arrived(arcv2.at[pl.ds(0, 7)], 8)
    sums = jnp.sum(arcv2[...], axis=0)
    whole_square = jnp.sum(jnp.where(lane1 == 0, sums, 0.0), axis=1, keepdims=True)
    whole_count = jnp.sum(jnp.where(lane1 == 1, sums, 0.0), axis=1, keepdims=True)
    level = whole_square / whole_count
    taps = detection_kernel[...].astype(F32)
    norm = jnp.sum(jnp.sum(taps * taps, axis=1, keepdims=True), axis=0, keepdims=True)
    noise[...] = jnp.broadcast_to(level, (1, PW))
    scale[...] = jnp.broadcast_to(1.0 / jnp.sqrt(1.0 + level * norm), (1, PW))
    sent(grcv.at[pl.ds(0, GROUP - 1)], 5)
    sent(arcv.at[pl.ds(0, GROUP - 1)], 6)
    sent(arcv2.at[pl.ds(0, 7)], 7)
    sent(db.at[pl.ds(0, dmargin)], 8)
    pltpu.make_async_copy(diffs, diffs, local.at[2]).wait()
    pltpu.make_async_copy(tf, tf, local.at[3]).wait()


def other_rows(ref, margin, c):
    return ref.at[pl.ds((1 - c) * (ROWS + margin), margin)]


def finish_kernel(difference, filtered, level, scale, out_difference, out_significance, noise, held, sums, factor, total, ins, outs):
    parts = [slice(r, r + 8) for r in range(0, ROWS, 8)]
    loads = [pltpu.make_async_copy(scale, factor, ins.at[0])]
    loads += [pltpu.make_async_copy(filtered.at[at], sums.at[at], ins.at[1 + i]) for i, at in enumerate(parts)]
    loads += [pltpu.make_async_copy(difference.at[at], held.at[at], ins.at[4 + i]) for i, at in enumerate(parts)]
    loads += [pltpu.make_async_copy(level, total, ins.at[7])]
    for load in loads:
        load.start()
    loads[0].wait()
    stores = []
    for i, at in enumerate(parts):
        loads[1 + i].wait()
        sums[at] = sums[at] * factor[0:1, 0:1]
        stores.append(pltpu.make_async_copy(sums.at[at], out_significance.at[at], outs.at[i]))
        stores[-1].start()
    for i, at in enumerate(parts):
        loads[4 + i].wait()
        stores.append(pltpu.make_async_copy(held.at[at], out_difference.at[at], outs.at[3 + i]))
        stores[-1].start()
    loads[7].wait()
    noise[...] = total[...]
    for store in stores:
        store.wait()


def on_device(
    exposure, row_shift, row_fraction, column_shift, column_fraction, piece_width,
    route_tile, route_cell, template, match_kernel, detection_kernel,
):
    vmem = pl.BlockSpec(memory_space=pltpu.VMEM)
    far = pl.BlockSpec(memory_space=pl.ANY)
    wide = template.shape[2]
    margin, dmargin = KS // 2, DK // 2
    difference, filtered, noise, scale = pl.pallas_call(
        kernel,
        out_shape=(
            jax.ShapeDtypeStruct((ROWS, wide), F32),
            jax.ShapeDtypeStruct((ROWS, wide), F32),
            jax.ShapeDtypeStruct((1, PW), F32),
            jax.ShapeDtypeStruct((1, PW), F32),
        ),
        in_specs=[far] * 11,
        out_specs=(far, far, vmem, vmem),
        scratch_shapes=[
            pltpu.VMEM((ROWS + HALO, NP, PW), F32),
            pltpu.VMEM((HALO, NP, PW), F32),
            pltpu.VMEM((ROWS, CAP, PW), F32),
            pltpu.VMEM((ROWS + 2 * margin, CAP, PW), BF16),
            pltpu.VMEM((ROWS, 1, PW), F32),
            pltpu.VMEM((NP, PW), F32),
            pltpu.VMEM((NP, PW), F32),
            pltpu.VMEM((GROUP, NP, PW), BF16),
            pltpu.VMEM((GROUP, NP, PW), BF16),
            pltpu.VMEM((NX - 1, GROUP, NP, PW), BF16),
            pltpu.VMEM((GROUP * CAP, PW), F32),
            pltpu.VMEM((GROUP, ROWS, PW), BF16),
            pltpu.VMEM((GROUP, ROWS, PW), BF16),
            pltpu.VMEM((NY * CAP, PW), F32),
            pltpu.VMEM((GROUP, ROWS, PW), BF16),
            pltpu.VMEM((GROUP, ROWS, PW), BF16),
            pltpu.VMEM((48 * 8, PW), F32),
            pltpu.VMEM((48 * 8, PW), F32),
            pltpu.VMEM(((KS + 1) * 2 * PW, 2 * PW), BF16),
            pltpu.VMEM(((DK + 1) * 2 * PW, 2 * PW), BF16),
            pltpu.VMEM((2, (ROWS // 2 + margin) * CAP, 2 * PW), BF16),
            pltpu.VMEM((2, (ROWS // 2 + dmargin) * CAP, 2 * PW), BF16),
            pltpu.VMEM((ROWS // 2 * CAP, 2 * PW), F32),
            pltpu.VMEM((ROWS, CAP, PW), F32),
            pltpu.VMEM((ROWS, CAP, PW), F32),
            pltpu.VMEM((ROWS + 2 * dmargin, CAP, PW), BF16),
            pltpu.VMEM((1, PW), F32),
            pltpu.VMEM((GROUP, 1, PW), F32),
            pltpu.VMEM((1, PW), F32),
            pltpu.VMEM((8, 1, PW), F32),
            pltpu.SemaphoreType.DMA((13,)),
            pltpu.SemaphoreType.DMA((9,)),
            pltpu.SemaphoreType.DMA((13,)),
            pltpu.SMEM((1,), I32),
            pltpu.SMEM((1,), I32),
            pltpu.VMEM((1, ROWS), BF16),
            pltpu.VMEM((1, NP * PW), BF16),
            pltpu.VMEM((1, NP), I32),
            pltpu.VMEM((1, NP), I32),
            pltpu.VMEM((1, NP), I32),
            pltpu.VMEM((KS, KS), BF16),
            pltpu.VMEM((DK, DK), BF16),
        ],
        compiler_params=pltpu.CompilerParams(collective_id=0, has_side_effects=True, vmem_limit_bytes=60 * 1024 * 1024),
        name="warp_match_detect",
    )(
        exposure[0], template[0], row_shift, column_shift, row_fraction, column_fraction,
        piece_width, route_tile, route_cell, match_kernel[0], detection_kernel[0],
    )
    difference, significance, noise = pl.pallas_call(
        finish_kernel,
        out_shape=(
            jax.ShapeDtypeStruct((ROWS, wide), F32),
            jax.ShapeDtypeStruct((ROWS, wide), F32),
            jax.ShapeDtypeStruct((1, PW), F32),
        ),
        in_specs=[far] * 4,
        out_specs=(far, far, vmem),
        scratch_shapes=[
            pltpu.VMEM((ROWS, wide), F32),
            pltpu.VMEM((ROWS, wide), F32),
            pltpu.VMEM((1, PW), F32),
            pltpu.VMEM((1, PW), F32),
            pltpu.SemaphoreType.DMA((8,)),
            pltpu.SemaphoreType.DMA((6,)),
        ],
        compiler_params=pltpu.CompilerParams(vmem_limit_bytes=60 * 1024 * 1024),
        name="finish",
    )(difference, filtered, noise, scale)
    return difference[None], significance[None], noise[0, 0]


def solution(mesh):
    finer = Mesh(
        mesh.devices.reshape(NZ, NX, NY, mesh.shape["row"]), ("ccd_0", "ccd_1", "ccd_2", "row")
    )
    placed = (
        P(CCD, "row", None),
        P(CCD),
        P(CCD, "row"),
        P(CCD),
        P(CCD, None),
        P(CCD, None),
        P(CCD, None),
        P(CCD, None),
        P(CCD, "row", None),
        P(CCD, None, None),
        P(CCD, None, None),
    )
    return jax.shard_map(
        on_device,
        mesh=finer,
        in_specs=placed,
        out_specs=(P(CCD, "row", None), P(CCD, "row", None), P()),
        check_vma=False,
    )
```

```python
import functools

import jax
import jax.numpy as jnp
from jax import lax
from jax.experimental import pallas as pl
from jax.experimental.pallas import tpu as pltpu
from jax.sharding import Mesh
from jax.sharding import PartitionSpec as P

PW = 128
HALO = 8
KS = 41
DK = 15
NZ, NX, NY = 8, 4, 4
GROUP = NZ * NY
NP = 16
CAP = 32
ROWS = 24
FR = ROWS // NZ
FL = PW // NY
EARLY = 5
MESH = pl.DeviceIdType.MESH
CCD = ("ccd_0", "ccd_1", "ccd_2")
F32, BF16, I32 = jnp.float32, jnp.bfloat16, jnp.int32


def lanes_of(shape):
    return lax.broadcasted_iota(I32, shape, len(shape) - 1)


def column_of(row, count):
    spread = jnp.broadcast_to(row, (count, count))
    pick = lax.broadcasted_iota(I32, (count, count), 0) == lanes_of((count, count))
    return jnp.sum(jnp.where(pick, spread, 0.0), axis=1, keepdims=True)


def down(x):
    rolled = pltpu.roll(x, 1, 0)
    return jnp.where(lax.broadcasted_iota(I32, x.shape, 0) == 0, 0.0, rolled)


def up(x):
    rolled = pltpu.roll(x, x.shape[0] - 1, 0)
    return jnp.where(lax.broadcasted_iota(I32, x.shape, 0) == x.shape[0] - 1, 0.0, rolled)


def band_bases(kernel_ref, extent, base_lo, base_hi, bands):
    depth = lax.broadcasted_iota(I32, (extent, 2 * PW), 0)
    place = lanes_of((extent, 2 * PW))
    picker = (lax.rem(depth + place, 2 * PW) == 0).astype(F32).astype(BF16)
    turned = jnp.dot(kernel_ref[...], picker, preferred_element_type=F32)
    for s in range(8):
        rolled = pltpu.roll(turned, s, 1) if s else turned
        base_lo[pl.ds(s, extent, stride=8), :] = rolled[:, :PW]
        base_hi[pl.ds(s, extent, stride=8), :] = rolled[:, PW:]
    bands[0:2 * PW, :] = jnp.zeros((2 * PW, PW), BF16)
    bands[(extent + 1) * 2 * PW:(extent + 2) * 2 * PW, :] = jnp.zeros((2 * PW, PW), BF16)


def build_bands(base_lo, base_hi, bands, extent, unroll):
    lane = lanes_of((8, PW))

    def step(a, carry):
        lo = base_lo[pl.ds(pl.multiple_of(a * 8, 8), 8), :]
        hi = base_hi[pl.ds(pl.multiple_of(a * 8, 8), 8), :]
        for pair in range(8):
            near, far = [], []
            for m in (2 * pair, 2 * pair + 1):
                shift = 8 * m
                rlo = pltpu.roll(lo, shift, 1) if shift else lo
                rhi = pltpu.roll(hi, shift, 1) if shift else hi
                near.append(jnp.where(lane >= shift, rlo, rhi))
                far.append(jnp.where(lane >= shift, rhi, rlo))
            for value, start in ((near, 16 * pair), (far, PW + 16 * pair)):
                at = pl.multiple_of((a + 1) * 2 * PW + start, 16)
                bands[pl.ds(at, 16), :] = jnp.concatenate(value, axis=0).astype(BF16)
        return carry

    lax.fori_loop(0, extent, step, 0, unroll=unroll)


def build_windows(rows_ref, start, count, margin, windows, unroll):
    lane = lanes_of((CAP, PW))

    def step(i, carry):
        r = start + i
        shifted = pltpu.roll(rows_ref[r].astype(F32), margin, 1)
        first = jnp.where(lane < margin, down(shifted), shifted)
        second = jnp.where(lane < margin, shifted, up(shifted))
        at = pl.ds(pl.multiple_of(r // 2 * CAP, CAP), CAP)
        windows[r % 2, at, 0:PW] = first.astype(BF16)
        windows[r % 2, at, PW:2 * PW] = second.astype(BF16)
        return carry

    lax.fori_loop(0, count, step, 0, unroll=unroll)


def clear_windows(start, count, windows):
    def step(i, carry):
        r = start + i
        at = pl.ds(pl.multiple_of(r // 2 * CAP, CAP), CAP)
        windows[r % 2, at, :] = jnp.zeros((CAP, 2 * PW), BF16)
        return carry

    lax.fori_loop(0, count, step, 0)


def near_first(i):
    half = (i + 1) // 2
    return lax.rem(half * (2 * (i % 2) - 1) + NZ, NZ)


def far_first(i):
    half = (i + 1) // 2
    return lax.rem(NZ // 2 + half * (1 - 2 * (i % 2)) + NZ, NZ)


def banded(windows, bands, per_step, first, last, total):
    half = ROWS // 2 * CAP

    def part(step):
        left = []
        for i in range(per_step):
            at = pl.ds(pl.multiple_of((step * per_step + i) * CAP, CAP), half)
            left += [windows[0, at, :], windows[1, at, :]]
        depth = per_step * 4 * PW
        at = pl.multiple_of(step * depth, depth)
        right = jnp.concatenate([bands[pl.ds(at + 2 * PW, depth), :], bands[pl.ds(at, depth), :]], axis=1)
        return jnp.dot(jnp.concatenate(left, axis=1), right, preferred_element_type=F32)

    if first == 0:
        total[...] = part(0)

    def step(i, carry):
        total[...] += part(i)
        return carry

    lax.fori_loop(max(first, 1), last, step, 0)


def kernel(
    exposure, template, *rest):
    row_shift, column_shift, small, rest = *rest[:2], rest[2:9], rest[9:]
    (difference, significance, stats,
    ext, hx, tf, tb, rfw, cfw, meta, msg, rcv, agb, acc, outg, grcv, held, mfr, mrc, alive,
    base_lo, base_hi, bands, dbands, windows, dwindows, total, matched, diffs, db,
    arsrc, arcv, ar2src, arcv2, numbers, local, sends, recvs,
    row_fraction, column_fraction, piece_width, route_tile, route_cell, match_kernel, detection_kernel) = rest
    z, x, y = (lax.axis_index(a) for a in CCD)
    c = lax.axis_index("row")
    me = z * NY + y

    def zpeer(dz, dy):
        pz = lax.rem(z + dz, NZ)
        py = lax.rem(y + dy, NY)
        return pz, py, {"ccd_0": pz, "ccd_2": py}

    def xpeer(dx, dc=0):
        return {"ccd_1": lax.rem(x + dx, NX), "row": lax.rem(c + dc, 2)}

    partner = {"row": 1 - c}
    near = [(dz, dy) for dz in range(NZ) for dy in range(NY) if dz or dy]
    across = [(dx, dc) for dx in range(NX) for dc in range(2) if dx or dc]

    def send(src, dst, stage, device, slot=None):
        pltpu.make_async_remote_copy(
            src_ref=src, dst_ref=dst, send_sem=sends.at[stage], recv_sem=recvs.at[stage if slot is None else slot],
            device_id=device, device_id_type=MESH,
        ).start()

    def arrived(ref, slot):
        pltpu.make_async_copy(ref, ref, recvs.at[slot]).wait()

    def sent(ref, stage):
        pltpu.make_async_copy(ref, ref, sends.at[stage]).wait()

    barrier = pltpu.get_barrier_semaphore()
    for dz, dy in near:
        pl.semaphore_signal(barrier, inc=1, device_id=zpeer(dz, dy)[2], device_id_type=MESH)
    for dx, dc in across:
        pl.semaphore_signal(barrier, inc=1, device_id=xpeer(dx, dc), device_id_type=MESH)
    held_small = (
        row_fraction, column_fraction, piece_width, route_tile, route_cell, match_kernel, detection_kernel,
    )
    loads = [pltpu.make_async_copy(src, dst, local.at[4 + i]) for i, (src, dst) in enumerate(zip(small, held_small))]
    for load in loads:
        load.start()
    for q in range(CAP):
        pltpu.make_async_copy(template.at[:, pl.ds(q * PW, PW)], tf.at[:, q, :], local.at[1]).start()
    for p in range(NP):
        pltpu.make_async_copy(exposure.at[:, pl.ds(p * PW, PW)], ext.at[pl.ds(0, ROWS), p, :], local.at[0]).start()
    for load in loads:
        load.wait()

    fractions = row_fraction[...].astype(F32)
    for r in range(ROWS):
        rfw[r] = jnp.broadcast_to(fractions[:, r:r + 1], (1, PW))
    columns = column_fraction[...].astype(F32)
    for p in range(NP):
        cfw[p:p + 1, :] = columns[:, p * PW:(p + 1) * PW]
    lane16 = lanes_of((NP, PW))
    width16 = column_of(piece_width[...].astype(F32), NP)
    tile16 = column_of(route_tile[...].astype(F32), NP)
    cell16 = column_of(route_cell[...].astype(F32), NP)
    meta[...] = jnp.where(lane16 == 96, tile16, jnp.where(lane16 == 97, cell16, jnp.where(lane16 == 98, width16, 0.0)))
    margin, dmargin = KS // 2, DK // 2
    pltpu.make_async_copy(tf, tf, local.at[1]).wait()

    def round_template(r, carry):
        tb[margin + r] = tf[r].astype(BF16)
        return carry

    lax.fori_loop(0, ROWS, round_template, 0, unroll=4)
    band_bases(match_kernel, KS, base_lo, base_hi, bands)
    build_bands(base_lo, base_hi, bands, KS, 4)
    clear_windows(c * (ROWS + margin), margin, windows)
    clear_windows(c * (ROWS + dmargin), dmargin, dwindows)
    pltpu.make_async_copy(ext.at[pl.ds(0, ROWS)], ext.at[pl.ds(0, ROWS)], local.at[0]).wait()
    t = jnp.max(row_shift[...].reshape(1, 1))
    s = jnp.max(column_shift[...].reshape(1, 1))
    left_turn = lax.rem(PW - s, PW)
    right_turn = PW - 1 - s
    weight = cfw[...]
    inside = lane16.astype(F32) < width16
    head = meta[...]

    def fragments(pz):
        rows = []
        for j in range(FR):
            r = pz * FR + j
            w = rfw[r]
            mixed = ((1.0 - w) * ext[r + t] + w * ext[r + t + 1]).astype(BF16).astype(F32)
            leftward = pltpu.roll(mixed, left_turn, 1)
            leftward = jnp.where(lane16 < PW - s, leftward, up(leftward))
            rightward = pltpu.roll(mixed, right_turn, 1)
            rightward = jnp.where(lane16 < PW - 1 - s, rightward, up(rightward))
            warped = (1.0 - weight) * leftward + weight * rightward
            rows.append(jnp.where(inside, warped, 0.0))
        out = []
        for py in range(NY):
            value = head
            for j in range(FR):
                turn = (FL * (j - py)) % PW
                moved = pltpu.roll(rows[j], turn, 1) if turn else rows[j]
                value = jnp.where((lane16 >= FL * j) & (lane16 < FL * (j + 1)), moved, value)
            out.append(value.astype(BF16))
        return out

    def place_fragments(pz):
        for py, value in enumerate(fragments(pz)):
            msg[pz * NY + py] = value

    def spread(pz):
        d = lax.rem(pz - z + NZ, NZ)
        dist = d + (NZ - 2 * d) * (d // 5)
        slot = 2 + (dist + 6) // 8 + (dist + 5) // 8
        for dy in range(NY):
            py = lax.rem(y + dy, NY)

            def go():
                send(msg.at[pz * NY + py], rcv.at[me], 2, {"ccd_0": pz, "ccd_2": py}, slot)

            if dy:
                go()
            else:
                pl.when(z != pz)(go)

    for pz in range(EARLY):
        place_fragments(pz)
    pl.semaphore_wait(barrier, len(near) + len(across))

    send(ext.at[pl.ds(0, HALO)], hx, 0, partner)
    send(tb.at[pl.ds(margin + (1 - c) * (ROWS - margin), margin)], tb.at[pl.ds(c * (ROWS + margin), margin)], 1, partner)
    for pz in range(EARLY):
        spread(pz)
    build_windows(tb, margin, ROWS, margin, windows, 4)
    arrived(hx, 0)
    keep = jnp.where(c == 0, 1.0, 0.0)
    for r in range(HALO):
        ext[ROWS + r] = hx[r] * keep

    for pz in range(EARLY, NZ):
        place_fragments(pz)
        spread(pz)
    rcv[me] = msg[me]

    def forward(slot, distances, count):
        arrived(rcv.at[pl.ds(0, count)], slot)
        for dz in distances:
            at = pl.ds(lax.rem(z + dz, NZ) * NY, NY)
            send(rcv.at[at], agb.at[0, at], 3, xpeer(1), slot=slot + 8)
            send(rcv.at[at], agb.at[2, at], 3, xpeer(3), slot=slot + 11)
            if slot > 2:
                send(rcv.at[at], agb.at[1, at], 3, xpeer(2), slot=16)

    def beside(group, count):
        taken = pl.ds(0, count * NY)
        arrived(agb.at[0, taken], 10 + group)
        arrived(agb.at[2, taken], 13 + group)

    def relay(distances):
        for dz in distances:
            start = lax.rem(z + dz, NZ) * NY
            low, high = pl.ds(start, NY // 2), pl.ds(start + NY // 2, NY // 2)
            send(agb.at[0, low], agb.at[1, low], 3, xpeer(1), slot=16)
            send(agb.at[2, high], agb.at[1, high], 3, xpeer(3), slot=16)

    arrived(other_rows(tb, margin, c), 1)
    build_windows(tb, (1 - c) * (ROWS + margin), margin, margin, windows, 4)
    banded(windows, bands, 3, 0, 4, total)
    forward(2, (0, 1, 7), 11)
    banded(windows, bands, 3, 4, 7, total)
    forward(3, (2, 6), 8)
    forward(4, (3, 5, 4), 12)

    def unpair(q, carry):
        at = pl.ds(pl.multiple_of(q * CAP, CAP), CAP)
        matched[2 * q] = total[at, 0:PW]
        matched[2 * q + 1] = total[at, PW:2 * PW]
        return carry

    lax.fori_loop(0, ROWS // 2, unpair, 0, unroll=2)
    lane24 = lanes_of((ROWS, PW))

    def split(pz):
        for py in range(NY):
            value, last = None, []
            for j in range(FR):
                turn = (FL * (j - py)) % PW
                row = matched[pz * FR + j]
                moved = pltpu.roll(row[:ROWS], turn, 1) if turn else row[:ROWS]
                value = moved if value is None else jnp.where(lane24 >= FL * j, moved, value)
                turn = (FL * (FR - py)) % PW
                last.append(pltpu.roll(row[ROWS:], turn, 1) if turn else row[ROWS:])
            value = jnp.where(lane24 >= FR * FL, jnp.concatenate(last, axis=0), value)
            mfr[pz * NY + py] = value.astype(BF16)

    def follow(i, carry):
        dz = far_first(i)
        pz = lax.rem(z + dz, NZ)
        split(pz)
        for dy in range(NY):
            _, py, device = zpeer(dz, dy)
            send(mfr.at[pz * NY + py], mrc.at[me], 4, device, 5)
        return carry

    lax.fori_loop(0, NZ - 1, follow, 0, unroll=7)
    split(z)
    for dy in range(1, NY):
        _, py, device = zpeer(0, dy)
        send(mfr.at[z * NY + py], mrc.at[me], 4, device, 5)
    mrc[me] = mfr[me]

    def codes(block):
        picks = (lanes_of((8, PW)) == lax.broadcasted_iota(I32, (8, PW), 0) + 96).astype(F32).astype(BF16)
        rows = lax.dot_general(picks, block, (((1,), (1,)), ((), ())), preferred_element_type=F32)
        tile = rows[0:1, :].astype(I32)
        cell = rows[1:2, :].astype(I32)
        tz, tx, ty = tile // (NX * NY), (tile // NY) % NX, tile % NY
        return jnp.where(tx == x, (tz * NY + ty) * CAP + cell, -1)

    chunk = NY * CAP
    chunk_rows = lax.broadcasted_iota(I32, (chunk, GROUP * NP), 0)

    def chosen(code, block, pz):
        hot = (chunk_rows == code - pz * chunk).astype(F32).astype(BF16)
        return jnp.dot(hot, block, preferred_element_type=F32)

    def flat(ref):
        return ref[...].reshape(GROUP * NP, PW)

    def add_block(block, first):
        code = codes(block)

        def step(pz, carry):
            at = pl.ds(pl.multiple_of(pz * chunk, chunk), chunk)
            value = chosen(code, block, pz)
            acc[at, :] = value if first else acc[at, :] + value
            return carry

        lax.fori_loop(0, NZ, step, 0, unroll=8)

    add_block(flat(rcv), True)
    beside(0, 3)
    relay((0, 1, 7))
    beside(1, 2)
    beside(2, 3)
    add_block(flat(agb.at[2]), False)
    add_block(flat(agb.at[0]), False)
    arrived(agb.at[1], 16)
    block = flat(agb.at[1])
    code = codes(block)
    lane8 = lanes_of((8, PW))

    def finish(pz):
        at = pl.ds(pl.multiple_of(pz * chunk, chunk), chunk)
        value = acc[at, :] + chosen(code, block, pz)
        acc[at, :] = value
        for py in range(NY):
            tile = value[py * CAP:(py + 1) * CAP]
            rows = []
            for j in range(FR):
                turn = (FL * (FR - j)) % PW
                rows.append(jnp.where(lane8 >= FR * FL, pltpu.roll(tile[ROWS:], turn, 1), tile[8 * j:8 * j + 8]))
            outg[pz * NY + py] = jnp.concatenate(rows, axis=0).astype(BF16)
        return value

    def deliver(i, carry):
        dz = far_first(i)
        pz = lax.rem(z + dz, NZ)
        finish(pz)
        for dy in range(NY):
            _, py, device = zpeer(dz, dy)
            send(outg.at[pz * NY + py], grcv.at[me], 5, device, 6)
        return carry

    lax.fori_loop(0, NZ - 1, deliver, 0, unroll=7)
    held[...] = finish(z)
    for dy in range(1, NY):
        _, py, device = zpeer(0, dy)
        send(outg.at[z * NY + py], grcv.at[me], 5, device, 6)
    grcv[me] = outg[me]

    lane32 = lanes_of((CAP, PW))
    own = held[pl.ds(pl.multiple_of(y * CAP, CAP), CAP), :]
    width32 = jnp.sum(jnp.where(lane32 == 98, own, 0.0), axis=1, keepdims=True)
    live = lane32.astype(F32) < width32
    live_count = ROWS * jnp.sum(width32, axis=0, keepdims=True)
    place = (lax.rem(lane24, FL) + FL * y).astype(F32)

    def mark_live(k, carry):
        value = acc[pl.ds(pl.multiple_of(k * CAP, CAP), CAP), :]
        width = jnp.sum(jnp.where(lane32 == 98, value, 0.0), axis=1, keepdims=True)
        last = jnp.concatenate([width[ROWS:]] * FR, axis=0)
        width = jnp.where(lane24 < FR * FL, width[:ROWS], last)
        alive[k] = jnp.where(place < width, 1.0, 0.0)
        return carry

    lax.fori_loop(0, GROUP, mark_live, 0, unroll=8)
    arrived(mrc.at[pl.ds(0, GROUP - 1)], 5)

    def square(k, squares):
        value = (outg[k].astype(F32) - mrc[k].astype(F32)) * alive[k]
        return squares + value * value

    squares = lax.fori_loop(0, GROUP, square, jnp.zeros((ROWS, PW), F32), unroll=8)
    square_sum = jnp.sum(jnp.sum(squares, axis=1, keepdims=True), axis=0, keepdims=True)
    lane1 = lanes_of((1, PW))
    arsrc[...] = jnp.where(lane1 == 0, square_sum, jnp.where(lane1 == 1, live_count, 0.0))
    for dx, dc in across:
        send(arsrc, arcv2.at[x * 2 + c], 6, xpeer(dx, dc), 7)
    arcv2[x * 2 + c] = arsrc[...]
    band_bases(detection_kernel, DK, base_lo, base_hi, dbands)
    build_bands(base_lo, base_hi, dbands, DK, 5)
    sent(rcv.at[pl.ds(0, GROUP - 1)], 2)
    sent(agb, 3)
    sent(hx, 0)
    sent(tb.at[pl.ds(0, margin)], 1)
    sent(mrc.at[pl.ds(0, GROUP - 1)], 4)
    arrived(arcv2.at[pl.ds(0, 7)], 7)
    ar2src[...] = jnp.sum(arcv2[...], axis=0)
    for dz, dy in near:
        send(ar2src, arcv.at[me], 7, zpeer(dz, dy)[2], 8)
    arcv[me] = ar2src[...]
    arrived(grcv.at[pl.ds(0, GROUP - 1)], 6)

    def subtract(pz, carry):
        parts = [grcv[pz * NY + py].astype(F32) for py in range(NY)]
        for j in range(FR):
            science = None
            for py in range(NY):
                turn = (FL * (py - j)) % PW
                moved = pltpu.roll(parts[py], turn, 1) if turn else parts[py]
                turn = (FL * (py - FR)) % PW
                rest = parts[py][8 * j:8 * j + 8]
                rest = pltpu.roll(rest, turn, 1) if turn else rest
                moved = jnp.concatenate([moved, rest], axis=0)
                science = moved if science is None else jnp.where(lane32 >= FL * py, moved, science)
            r = pz * FR + j
            value = jnp.where(live, science - matched[r], 0.0)
            diffs[r] = value
            db[dmargin + r] = value.astype(BF16)
        return carry

    lax.fori_loop(0, NZ, subtract, 0, unroll=4)
    send(db.at[pl.ds(dmargin + (1 - c) * (ROWS - dmargin), dmargin)], db.at[pl.ds(c * (ROWS + dmargin), dmargin)], 8, partner, 9)
    for q in range(CAP):
        pltpu.make_async_copy(diffs.at[:, q, :], difference.at[:, pl.ds(q * PW, PW)], local.at[2]).start()
    build_windows(db, dmargin, ROWS, dmargin, dwindows, 4)

    arrived(other_rows(db, dmargin, c), 9)
    build_windows(db, (1 - c) * (ROWS + dmargin), dmargin, dmargin, dwindows, 7)
    banded(dwindows, dbands, 4, 0, (DK + 1) // 8, total)

    def unpair_filtered(q, carry):
        at = pl.ds(pl.multiple_of(q * CAP, CAP), CAP)
        tf[2 * q] = total[at, 0:PW]
        tf[2 * q + 1] = total[at, PW:2 * PW]
        return carry

    lax.fori_loop(0, ROWS // 2, unpair_filtered, 0, unroll=6)
    for q in range(CAP):
        pltpu.make_async_copy(tf.at[:, q, :], significance.at[:, pl.ds(q * PW, PW)], local.at[3]).start()
    arrived(arcv.at[pl.ds(0, GROUP - 1)], 8)
    sums = jnp.sum(arcv[...], axis=0)
    whole_square = jnp.sum(jnp.where(lane1 == 0, sums, 0.0), axis=1, keepdims=True)
    whole_count = jnp.sum(jnp.where(lane1 == 1, sums, 0.0), axis=1, keepdims=True)
    level = whole_square / whole_count
    taps = detection_kernel[...].astype(F32)
    norm = jnp.sum(jnp.sum(taps * taps, axis=1, keepdims=True), axis=0, keepdims=True)
    second = lax.broadcasted_iota(I32, (8, PW), 0) == 1
    numbers[...] = jnp.where(second, 1.0 / jnp.sqrt(1.0 + level * norm), level)
    report = pltpu.make_async_copy(numbers, stats, local.at[4])
    report.start()
    sent(grcv.at[pl.ds(0, GROUP - 1)], 5)
    sent(arcv2.at[pl.ds(0, 7)], 6)
    sent(arcv.at[pl.ds(0, GROUP - 1)], 7)
    sent(db.at[pl.ds(0, dmargin)], 8)
    pltpu.make_async_copy(diffs, diffs, local.at[2]).wait()
    pltpu.make_async_copy(tf, tf, local.at[3]).wait()
    report.wait()


def other_rows(ref, margin, c):
    return ref.at[pl.ds((1 - c) * (ROWS + margin), margin)]


def finish_kernel(difference, filtered, stats, out_difference, out_significance, out_noise, held, sums, numbers, ins, outs):
    loads = [
        pltpu.make_async_copy(stats, numbers, ins.at[0]),
        pltpu.make_async_copy(filtered, sums, ins.at[1]),
        pltpu.make_async_copy(difference, held, ins.at[2]),
    ]
    stores = [
        pltpu.make_async_copy(numbers.at[pl.ds(0, 1)], out_noise, outs.at[0]),
        pltpu.make_async_copy(sums, out_significance, outs.at[1]),
        pltpu.make_async_copy(held, out_difference, outs.at[2]),
    ]
    for load in loads:
        load.start()
    loads[0].wait()
    stores[0].start()
    loads[1].wait()
    sums[...] = sums[...] * numbers[1:2, 0:1]
    stores[1].start()
    loads[2].wait()
    stores[2].start()
    for store in stores:
        store.wait()


def on_device(
    exposure, row_shift, row_fraction, column_shift, column_fraction, piece_width,
    route_tile, route_cell, template, match_kernel, detection_kernel,
):
    vmem = pl.BlockSpec(memory_space=pltpu.VMEM)
    far = pl.BlockSpec(memory_space=pl.ANY)
    wide = template.shape[2]
    margin, dmargin = KS // 2, DK // 2
    difference, filtered, stats = pl.pallas_call(
        kernel,
        out_shape=(
            jax.ShapeDtypeStruct((ROWS, wide), F32),
            jax.ShapeDtypeStruct((ROWS, wide), F32),
            jax.ShapeDtypeStruct((8, PW), F32),
        ),
        in_specs=[far, far, vmem, vmem] + [far] * 7,
        out_specs=(far, far, far),
        scratch_shapes=[
            pltpu.VMEM((ROWS + HALO, NP, PW), F32),
            pltpu.VMEM((HALO, NP, PW), F32),
            pltpu.VMEM((ROWS, CAP, PW), F32),
            pltpu.VMEM((ROWS + 2 * margin, CAP, PW), BF16),
            pltpu.VMEM((ROWS, 1, PW), F32),
            pltpu.VMEM((NP, PW), F32),
            pltpu.VMEM((NP, PW), F32),
            pltpu.VMEM((GROUP, NP, PW), BF16),
            pltpu.VMEM((GROUP, NP, PW), BF16),
            pltpu.VMEM((NX - 1, GROUP, NP, PW), BF16),
            pltpu.VMEM((GROUP * CAP, PW), F32),
            pltpu.VMEM((GROUP, ROWS, PW), BF16),
            pltpu.VMEM((GROUP, ROWS, PW), BF16),
            pltpu.VMEM((NY * CAP, PW), F32),
            pltpu.VMEM((GROUP, ROWS, PW), BF16),
            pltpu.VMEM((GROUP, ROWS, PW), BF16),
            pltpu.VMEM((GROUP, ROWS, PW), F32),
            pltpu.VMEM((48 * 8, PW), F32),
            pltpu.VMEM((48 * 8, PW), F32),
            pltpu.VMEM(((KS + 2) * 2 * PW, PW), BF16),
            pltpu.VMEM(((DK + 2) * 2 * PW, PW), BF16),
            pltpu.VMEM((2, (ROWS // 2 + margin) * CAP, 2 * PW), BF16),
            pltpu.VMEM((2, (ROWS // 2 + dmargin) * CAP, 2 * PW), BF16),
            pltpu.VMEM((ROWS // 2 * CAP, 2 * PW), F32),
            pltpu.VMEM((ROWS, CAP, PW), F32),
            pltpu.VMEM((ROWS, CAP, PW), F32),
            pltpu.VMEM((ROWS + 2 * dmargin, CAP, PW), BF16),
            pltpu.VMEM((1, PW), F32),
            pltpu.VMEM((GROUP, 1, PW), F32),
            pltpu.VMEM((1, PW), F32),
            pltpu.VMEM((8, 1, PW), F32),
            pltpu.VMEM((8, PW), F32),
            pltpu.SemaphoreType.DMA((13,)),
            pltpu.SemaphoreType.DMA((9,)),
            pltpu.SemaphoreType.DMA((17,)),
            pltpu.VMEM((1, ROWS), BF16),
            pltpu.VMEM((1, NP * PW), BF16),
            pltpu.VMEM((1, NP), I32),
            pltpu.VMEM((1, NP), I32),
            pltpu.VMEM((1, NP), I32),
            pltpu.VMEM((KS, KS), BF16),
            pltpu.VMEM((DK, DK), BF16),
        ],
        compiler_params=pltpu.CompilerParams(collective_id=0, has_side_effects=True, vmem_limit_bytes=60 * 1024 * 1024),
        name="warp_match_detect",
    )(
        exposure[0], template[0], row_shift, column_shift, row_fraction, column_fraction,
        piece_width, route_tile, route_cell, match_kernel[0], detection_kernel[0],
    )
    difference, significance, noise = pl.pallas_call(
        finish_kernel,
        out_shape=(
            jax.ShapeDtypeStruct((ROWS, wide), F32),
            jax.ShapeDtypeStruct((ROWS, wide), F32),
            jax.ShapeDtypeStruct((1, PW), F32),
        ),
        in_specs=[far] * 3,
        out_specs=(far, far, far),
        scratch_shapes=[
            pltpu.VMEM((ROWS, wide), F32),
            pltpu.VMEM((ROWS, wide), F32),
            pltpu.VMEM((8, PW), F32),
            pltpu.SemaphoreType.DMA((3,)),
            pltpu.SemaphoreType.DMA((3,)),
        ],
        compiler_params=pltpu.CompilerParams(vmem_limit_bytes=60 * 1024 * 1024),
        name="finish",
    )(difference, filtered, stats)
    return difference[None], significance[None], noise[0, 0]


def solution(mesh):
    finer = Mesh(
        mesh.devices.reshape(NZ, NX, NY, mesh.shape["row"]), ("ccd_0", "ccd_1", "ccd_2", "row")
    )
    placed = (
        P(CCD, "row", None),
        P(CCD),
        P(CCD, "row"),
        P(CCD),
        P(CCD, None),
        P(CCD, None),
        P(CCD, None),
        P(CCD, None),
        P(CCD, "row", None),
        P(CCD, None, None),
        P(CCD, None, None),
    )
    return jax.shard_map(
        on_device,
        mesh=finer,
        in_specs=placed,
        out_specs=(P(CCD, "row", None), P(CCD, "row", None), P()),
        check_vma=False,
    )
```

```python
import functools

import jax
import jax.numpy as jnp
from jax import lax
from jax.experimental import pallas as pl
from jax.experimental.pallas import tpu as pltpu
from jax.sharding import Mesh
from jax.sharding import PartitionSpec as P

PW = 128
HALO = 8
KS = 41
DK = 15
NZ, NX, NY = 8, 4, 4
GROUP = NZ * NY
NP = 16
CAP = 32
ROWS = 24
FR = ROWS // NZ
FL = PW // NY
EARLY = 5
MESH = pl.DeviceIdType.MESH
CCD = ("ccd_0", "ccd_1", "ccd_2")
F32, BF16, I32 = jnp.float32, jnp.bfloat16, jnp.int32


def lanes_of(shape):
    return lax.broadcasted_iota(I32, shape, len(shape) - 1)


def column_of(row, count):
    spread = jnp.broadcast_to(row, (count, count))
    pick = lax.broadcasted_iota(I32, (count, count), 0) == lanes_of((count, count))
    return jnp.sum(jnp.where(pick, spread, 0.0), axis=1, keepdims=True)


def down(x):
    rolled = pltpu.roll(x, 1, 0)
    return jnp.where(lax.broadcasted_iota(I32, x.shape, 0) == 0, 0.0, rolled)


def up(x):
    rolled = pltpu.roll(x, x.shape[0] - 1, 0)
    return jnp.where(lax.broadcasted_iota(I32, x.shape, 0) == x.shape[0] - 1, 0.0, rolled)


def band_bases(kernel_ref, extent, base_lo, base_hi, bands):
    depth = lax.broadcasted_iota(I32, (extent, 2 * PW), 0)
    place = lanes_of((extent, 2 * PW))
    picker = (lax.rem(depth + place, 2 * PW) == 0).astype(F32).astype(BF16)
    turned = jnp.dot(kernel_ref[...], picker, preferred_element_type=F32)
    for s in range(8):
        rolled = pltpu.roll(turned, s, 1) if s else turned
        base_lo[pl.ds(s, extent, stride=8), :] = rolled[:, :PW]
        base_hi[pl.ds(s, extent, stride=8), :] = rolled[:, PW:]
    bands[0:2 * PW, :] = jnp.zeros((2 * PW, PW), BF16)
    bands[(extent + 1) * 2 * PW:(extent + 2) * 2 * PW, :] = jnp.zeros((2 * PW, PW), BF16)


def build_bands(base_lo, base_hi, bands, extent, unroll):
    lane = lanes_of((8, PW))

    def step(a, carry):
        lo = base_lo[pl.ds(pl.multiple_of(a * 8, 8), 8), :]
        hi = base_hi[pl.ds(pl.multiple_of(a * 8, 8), 8), :]
        for pair in range(8):
            near, far = [], []
            for m in (2 * pair, 2 * pair + 1):
                shift = 8 * m
                rlo = pltpu.roll(lo, shift, 1) if shift else lo
                rhi = pltpu.roll(hi, shift, 1) if shift else hi
                near.append(jnp.where(lane >= shift, rlo, rhi))
                far.append(jnp.where(lane >= shift, rhi, rlo))
            for value, start in ((near, 16 * pair), (far, PW + 16 * pair)):
                at = pl.multiple_of((a + 1) * 2 * PW + start, 16)
                bands[pl.ds(at, 16), :] = jnp.concatenate(value, axis=0).astype(BF16)
        return carry

    lax.fori_loop(0, extent, step, 0, unroll=unroll)


def build_windows(rows_ref, start, count, margin, windows, unroll):
    lane = lanes_of((CAP, PW))

    def step(i, carry):
        r = start + i
        shifted = pltpu.roll(rows_ref[r].astype(F32), margin, 1)
        first = jnp.where(lane < margin, down(shifted), shifted)
        second = jnp.where(lane < margin, shifted, up(shifted))
        at = pl.ds(pl.multiple_of(r // 2 * CAP, CAP), CAP)
        windows[r % 2, at, 0:PW] = first.astype(BF16)
        windows[r % 2, at, PW:2 * PW] = second.astype(BF16)
        return carry

    lax.fori_loop(0, count, step, 0, unroll=unroll)


def clear_windows(start, count, windows):
    def step(i, carry):
        r = start + i
        at = pl.ds(pl.multiple_of(r // 2 * CAP, CAP), CAP)
        windows[r % 2, at, :] = jnp.zeros((CAP, 2 * PW), BF16)
        return carry

    lax.fori_loop(0, count, step, 0)


def rows_of(pz):
    return pz * 3 % NZ if isinstance(pz, int) else lax.rem(pz * 3, NZ)


def far_first(i):
    half = (i + 1) // 2
    return lax.rem(NZ // 2 + half * (1 - 2 * (i % 2)) + NZ, NZ)


def banded(windows, bands, per_step, first, last, total):
    half = ROWS // 2 * CAP

    def part(step):
        left = []
        for i in range(per_step):
            at = pl.ds(pl.multiple_of((step * per_step + i) * CAP, CAP), half)
            left += [windows[0, at, :], windows[1, at, :]]
        depth = per_step * 4 * PW
        at = pl.multiple_of(step * depth, depth)
        right = jnp.concatenate([bands[pl.ds(at + 2 * PW, depth), :], bands[pl.ds(at, depth), :]], axis=1)
        return jnp.dot(jnp.concatenate(left, axis=1), right, preferred_element_type=F32)

    if first == 0:
        total[...] = part(0)

    def step(i, carry):
        total[...] += part(i)
        return carry

    lax.fori_loop(max(first, 1), last, step, 0)


def kernel(
    exposure, template, *rest):
    row_shift, column_shift, small, rest = *rest[:2], rest[2:9], rest[9:]
    (difference, significance, stats,
    ext, hx, tf, tb, rfw, cfw, meta, msg, rcv, agb, acc, outg, grcv, held, mfr, mrc, alive,
    base_lo, base_hi, bands, dbands, windows, dwindows, total, matched, diffs, db,
    arsrc, arcv, ar2src, arcv2, numbers, local, sends, recvs,
    row_fraction, column_fraction, piece_width, route_tile, route_cell, match_kernel, detection_kernel) = rest
    z, x, y = (lax.axis_index(a) for a in CCD)
    c = lax.axis_index("row")
    me = z * NY + y

    def zpeer(dz, dy):
        pz = lax.rem(z + dz, NZ)
        py = lax.rem(y + dy, NY)
        return pz, py, {"ccd_0": pz, "ccd_2": py}

    def xpeer(dx, dc=0):
        return {"ccd_1": lax.rem(x + dx, NX), "row": lax.rem(c + dc, 2)}

    partner = {"row": 1 - c}
    near = [(dz, dy) for dz in range(NZ) for dy in range(NY) if dz or dy]
    across = [(dx, dc) for dx in range(NX) for dc in range(2) if dx or dc]

    def send(src, dst, stage, device, slot=None):
        pltpu.make_async_remote_copy(
            src_ref=src, dst_ref=dst, send_sem=sends.at[stage], recv_sem=recvs.at[stage if slot is None else slot],
            device_id=device, device_id_type=MESH,
        ).start()

    def arrived(ref, slot):
        pltpu.make_async_copy(ref, ref, recvs.at[slot]).wait()

    def sent(ref, stage):
        pltpu.make_async_copy(ref, ref, sends.at[stage]).wait()

    barrier = pltpu.get_barrier_semaphore()
    for dz, dy in near:
        pl.semaphore_signal(barrier, inc=1, device_id=zpeer(dz, dy)[2], device_id_type=MESH)
    for dx, dc in across:
        pl.semaphore_signal(barrier, inc=1, device_id=xpeer(dx, dc), device_id_type=MESH)
    held_small = (
        row_fraction, column_fraction, piece_width, route_tile, route_cell, match_kernel, detection_kernel,
    )
    loads = [pltpu.make_async_copy(src, dst, local.at[4 + i]) for i, (src, dst) in enumerate(zip(small, held_small))]
    for load in loads:
        load.start()
    for q in range(CAP):
        pltpu.make_async_copy(template.at[:, pl.ds(q * PW, PW)], tf.at[:, q, :], local.at[1]).start()
    for p in range(NP):
        pltpu.make_async_copy(exposure.at[:, pl.ds(p * PW, PW)], ext.at[pl.ds(0, ROWS), p, :], local.at[0]).start()
    for load in loads:
        load.wait()

    fractions = row_fraction[...].astype(F32)
    for r in range(ROWS):
        rfw[r] = jnp.broadcast_to(fractions[:, r:r + 1], (1, PW))
    columns = column_fraction[...].astype(F32)
    for p in range(NP):
        cfw[p:p + 1, :] = columns[:, p * PW:(p + 1) * PW]
    lane16 = lanes_of((NP, PW))
    width16 = column_of(piece_width[...].astype(F32), NP)
    tile16 = column_of(route_tile[...].astype(F32), NP)
    cell16 = column_of(route_cell[...].astype(F32), NP)
    meta[...] = jnp.where(lane16 == 96, tile16, jnp.where(lane16 == 97, cell16, jnp.where(lane16 == 98, width16, 0.0)))
    margin, dmargin = KS // 2, DK // 2
    pltpu.make_async_copy(tf, tf, local.at[1]).wait()

    def round_template(r, carry):
        tb[margin + r] = tf[r].astype(BF16)
        return carry

    lax.fori_loop(0, ROWS, round_template, 0, unroll=4)
    band_bases(match_kernel, KS, base_lo, base_hi, bands)
    build_bands(base_lo, base_hi, bands, KS, 4)
    clear_windows(c * (ROWS + margin), margin, windows)
    clear_windows(c * (ROWS + dmargin), dmargin, dwindows)
    pltpu.make_async_copy(ext.at[pl.ds(0, ROWS)], ext.at[pl.ds(0, ROWS)], local.at[0]).wait()
    t = jnp.max(row_shift[...].reshape(1, 1))
    s = jnp.max(column_shift[...].reshape(1, 1))
    left_turn = lax.rem(PW - s, PW)
    right_turn = PW - 1 - s
    weight = cfw[...]
    inside = lane16.astype(F32) < width16
    head = meta[...]

    def fragments(group):
        rows = []
        for j in range(FR):
            r = group * FR + j
            w = rfw[r]
            mixed = ((1.0 - w) * ext[r + t] + w * ext[r + t + 1]).astype(BF16).astype(F32)
            leftward = pltpu.roll(mixed, left_turn, 1)
            leftward = jnp.where(lane16 < PW - s, leftward, up(leftward))
            rightward = pltpu.roll(mixed, right_turn, 1)
            rightward = jnp.where(lane16 < PW - 1 - s, rightward, up(rightward))
            warped = (1.0 - weight) * leftward + weight * rightward
            rows.append(jnp.where(inside, warped, 0.0))
        out = []
        for py in range(NY):
            value = head
            for j in range(FR):
                turn = (FL * (j - py)) % PW
                moved = pltpu.roll(rows[j], turn, 1) if turn else rows[j]
                value = jnp.where((lane16 >= FL * j) & (lane16 < FL * (j + 1)), moved, value)
            out.append(value.astype(BF16))
        return out

    def place_fragments(pz):
        for py, value in enumerate(fragments(rows_of(pz))):
            msg[pz * NY + py] = value

    def spread(pz):
        d = lax.rem(pz - z + NZ, NZ)
        dist = d + (NZ - 2 * d) * (d // 5)
        slot = 2 + (dist + 6) // 8 + (dist + 5) // 8
        for dy in range(NY):
            py = lax.rem(y + dy, NY)

            def go():
                send(msg.at[pz * NY + py], rcv.at[me], 2, {"ccd_0": pz, "ccd_2": py}, slot)

            if dy:
                go()
            else:
                pl.when(z != pz)(go)

    planes = [rows_of(group) for group in range(NZ)]
    for pz in planes[:EARLY]:
        place_fragments(pz)
    pl.semaphore_wait(barrier, len(near) + len(across))

    send(ext.at[pl.ds(0, HALO)], hx, 0, partner)
    send(tb.at[pl.ds(margin + (1 - c) * (ROWS - margin), margin)], tb.at[pl.ds(c * (ROWS + margin), margin)], 1, partner)
    for pz in planes[:EARLY]:
        spread(pz)
    build_windows(tb, margin, ROWS, margin, windows, 4)
    arrived(hx, 0)
    keep = jnp.where(c == 0, 1.0, 0.0)
    for r in range(HALO):
        ext[ROWS + r] = hx[r] * keep

    for pz in planes[EARLY:]:
        place_fragments(pz)
        spread(pz)
    rcv[me] = msg[me]

    def forward(slot, distances, count):
        arrived(rcv.at[pl.ds(0, count)], slot)
        for dz in distances:
            at = pl.ds(lax.rem(z + dz, NZ) * NY, NY)
            send(rcv.at[at], agb.at[0, at], 3, xpeer(1), slot=slot + 8)
            send(rcv.at[at], agb.at[2, at], 3, xpeer(3), slot=slot + 11)
            if slot > 2:
                send(rcv.at[at], agb.at[1, at], 3, xpeer(2), slot=16)

    def beside(group, count):
        taken = pl.ds(0, count * NY)
        arrived(agb.at[0, taken], 10 + group)
        arrived(agb.at[2, taken], 13 + group)

    def relay(distances):
        for dz in distances:
            start = lax.rem(z + dz, NZ) * NY
            low, high = pl.ds(start, NY // 2), pl.ds(start + NY // 2, NY // 2)
            send(agb.at[0, low], agb.at[1, low], 3, xpeer(1), slot=16)
            send(agb.at[2, high], agb.at[1, high], 3, xpeer(3), slot=16)

    arrived(other_rows(tb, margin, c), 1)
    build_windows(tb, (1 - c) * (ROWS + margin), margin, margin, windows, 4)
    banded(windows, bands, 3, 0, 7, total)
    forward(2, (0, 1, 7), 11)

    def unpair(q, carry):
        at = pl.ds(pl.multiple_of(q * CAP, CAP), CAP)
        matched[2 * q] = total[at, 0:PW]
        matched[2 * q + 1] = total[at, PW:2 * PW]
        return carry

    lax.fori_loop(0, ROWS // 2, unpair, 0, unroll=2)
    lane24 = lanes_of((ROWS, PW))

    def split(pz):
        for py in range(NY):
            value, last = None, []
            for j in range(FR):
                turn = (FL * (j - py)) % PW
                row = matched[rows_of(pz) * FR + j]
                moved = pltpu.roll(row[:ROWS], turn, 1) if turn else row[:ROWS]
                value = moved if value is None else jnp.where(lane24 >= FL * j, moved, value)
                turn = (FL * (FR - py)) % PW
                last.append(pltpu.roll(row[ROWS:], turn, 1) if turn else row[ROWS:])
            value = jnp.where(lane24 >= FR * FL, jnp.concatenate(last, axis=0), value)
            mfr[pz * NY + py] = value.astype(BF16)

    def follow(i, carry):
        dz = far_first(i)
        pz = lax.rem(z + dz, NZ)
        split(pz)
        for dy in range(NY):
            _, py, device = zpeer(dz, dy)
            send(mfr.at[pz * NY + py], mrc.at[me], 4, device, 5)
        return carry

    lax.fori_loop(0, NZ - 1, follow, 0, unroll=7)
    split(z)
    for dy in range(1, NY):
        _, py, device = zpeer(0, dy)
        send(mfr.at[z * NY + py], mrc.at[me], 4, device, 5)
    mrc[me] = mfr[me]
    forward(3, (2, 6), 8)
    forward(4, (3, 5, 4), 12)

    def codes(block):
        picks = (lanes_of((8, PW)) == lax.broadcasted_iota(I32, (8, PW), 0) + 96).astype(F32).astype(BF16)
        rows = lax.dot_general(picks, block, (((1,), (1,)), ((), ())), preferred_element_type=F32)
        tile = rows[0:1, :].astype(I32)
        cell = rows[1:2, :].astype(I32)
        tz, tx, ty = tile // (NX * NY), (tile // NY) % NX, tile % NY
        return jnp.where(tx == x, (tz * NY + ty) * CAP + cell, -1)

    chunk = NY * CAP
    chunk_rows = lax.broadcasted_iota(I32, (chunk, GROUP * NP), 0)

    def chosen(code, block, pz):
        hot = (chunk_rows == code - pz * chunk).astype(F32).astype(BF16)
        return jnp.dot(hot, block, preferred_element_type=F32)

    def flat(ref):
        return ref[...].reshape(GROUP * NP, PW)

    def add_block(block, first):
        code = codes(block)

        def step(pz, carry):
            at = pl.ds(pl.multiple_of(pz * chunk, chunk), chunk)
            value = chosen(code, block, pz)
            acc[at, :] = value if first else acc[at, :] + value
            return carry

        lax.fori_loop(0, NZ, step, 0, unroll=8)

    add_block(flat(rcv), True)
    beside(0, 3)
    relay((0, 1, 7))
    beside(1, 2)
    beside(2, 3)
    add_block(flat(agb.at[2]), False)
    add_block(flat(agb.at[0]), False)
    arrived(agb.at[1], 16)
    block = flat(agb.at[1])
    code = codes(block)
    lane8 = lanes_of((8, PW))

    def finish(pz):
        at = pl.ds(pl.multiple_of(pz * chunk, chunk), chunk)
        value = acc[at, :] + chosen(code, block, pz)
        acc[at, :] = value
        for py in range(NY):
            tile = value[py * CAP:(py + 1) * CAP]
            rows = []
            for j in range(FR):
                turn = (FL * (FR - j)) % PW
                rows.append(jnp.where(lane8 >= FR * FL, pltpu.roll(tile[ROWS:], turn, 1), tile[8 * j:8 * j + 8]))
            outg[pz * NY + py] = jnp.concatenate(rows, axis=0).astype(BF16)
        return value

    def deliver(i, carry):
        dz = far_first(i)
        pz = lax.rem(z + dz, NZ)
        finish(pz)
        for dy in range(NY):
            _, py, device = zpeer(dz, dy)
            send(outg.at[pz * NY + py], grcv.at[me], 5, device, 6)
        return carry

    lax.fori_loop(0, NZ - 1, deliver, 0, unroll=7)
    held[...] = finish(z)
    for dy in range(1, NY):
        _, py, device = zpeer(0, dy)
        send(outg.at[z * NY + py], grcv.at[me], 5, device, 6)
    grcv[me] = outg[me]

    lane32 = lanes_of((CAP, PW))
    own = held[pl.ds(pl.multiple_of(y * CAP, CAP), CAP), :]
    width32 = jnp.sum(jnp.where(lane32 == 98, own, 0.0), axis=1, keepdims=True)
    live = lane32.astype(F32) < width32
    live_count = ROWS * jnp.sum(width32, axis=0, keepdims=True)
    place = (lax.rem(lane24, FL) + FL * y).astype(F32)

    def mark_live(k, carry):
        value = acc[pl.ds(pl.multiple_of(k * CAP, CAP), CAP), :]
        width = jnp.sum(jnp.where(lane32 == 98, value, 0.0), axis=1, keepdims=True)
        last = jnp.concatenate([width[ROWS:]] * FR, axis=0)
        width = jnp.where(lane24 < FR * FL, width[:ROWS], last)
        alive[k] = jnp.where(place < width, 1.0, 0.0)
        return carry

    lax.fori_loop(0, GROUP, mark_live, 0, unroll=8)
    arrived(mrc.at[pl.ds(0, GROUP - 1)], 5)

    def square(k, squares):
        value = (outg[k].astype(F32) - mrc[k].astype(F32)) * alive[k]
        return squares + value * value

    squares = lax.fori_loop(0, GROUP, square, jnp.zeros((ROWS, PW), F32), unroll=8)
    square_sum = jnp.sum(jnp.sum(squares, axis=1, keepdims=True), axis=0, keepdims=True)
    lane1 = lanes_of((1, PW))
    arsrc[...] = jnp.where(lane1 == 0, square_sum, jnp.where(lane1 == 1, live_count, 0.0))
    for dx, dc in across:
        send(arsrc, arcv2.at[x * 2 + c], 6, xpeer(dx, dc), 7)
    arcv2[x * 2 + c] = arsrc[...]
    band_bases(detection_kernel, DK, base_lo, base_hi, dbands)
    build_bands(base_lo, base_hi, dbands, DK, 5)
    sent(rcv.at[pl.ds(0, GROUP - 1)], 2)
    sent(agb, 3)
    sent(hx, 0)
    sent(tb.at[pl.ds(0, margin)], 1)
    sent(mrc.at[pl.ds(0, GROUP - 1)], 4)
    arrived(arcv2.at[pl.ds(0, 7)], 7)
    ar2src[...] = jnp.sum(arcv2[...], axis=0)
    for dz, dy in near:
        send(ar2src, arcv.at[me], 7, zpeer(dz, dy)[2], 8)
    arcv[me] = ar2src[...]
    arrived(grcv.at[pl.ds(0, GROUP - 1)], 6)

    def subtract(pz, carry):
        parts = [grcv[pz * NY + py].astype(F32) for py in range(NY)]
        for j in range(FR):
            science = None
            for py in range(NY):
                turn = (FL * (py - j)) % PW
                moved = pltpu.roll(parts[py], turn, 1) if turn else parts[py]
                turn = (FL * (py - FR)) % PW
                rest = parts[py][8 * j:8 * j + 8]
                rest = pltpu.roll(rest, turn, 1) if turn else rest
                moved = jnp.concatenate([moved, rest], axis=0)
                science = moved if science is None else jnp.where(lane32 >= FL * py, moved, science)
            r = rows_of(pz) * FR + j
            value = jnp.where(live, science - matched[r], 0.0)
            diffs[r] = value
            db[dmargin + r] = value.astype(BF16)
        return carry

    lax.fori_loop(0, NZ, subtract, 0, unroll=4)
    send(db.at[pl.ds(dmargin + (1 - c) * (ROWS - dmargin), dmargin)], db.at[pl.ds(c * (ROWS + dmargin), dmargin)], 8, partner, 9)
    for q in range(CAP):
        pltpu.make_async_copy(diffs.at[:, q, :], difference.at[:, pl.ds(q * PW, PW)], local.at[2]).start()
    build_windows(db, dmargin, ROWS, dmargin, dwindows, 4)

    arrived(other_rows(db, dmargin, c), 9)
    build_windows(db, (1 - c) * (ROWS + dmargin), dmargin, dmargin, dwindows, 7)
    banded(dwindows, dbands, 4, 0, (DK + 1) // 8, total)

    def unpair_filtered(q, carry):
        at = pl.ds(pl.multiple_of(q * CAP, CAP), CAP)
        tf[2 * q] = total[at, 0:PW]
        tf[2 * q + 1] = total[at, PW:2 * PW]
        return carry

    lax.fori_loop(0, ROWS // 2, unpair_filtered, 0, unroll=6)
    for q in range(CAP):
        pltpu.make_async_copy(tf.at[:, q, :], significance.at[:, pl.ds(q * PW, PW)], local.at[3]).start()
    arrived(arcv.at[pl.ds(0, GROUP - 1)], 8)
    sums = jnp.sum(arcv[...], axis=0)
    whole_square = jnp.sum(jnp.where(lane1 == 0, sums, 0.0), axis=1, keepdims=True)
    whole_count = jnp.sum(jnp.where(lane1 == 1, sums, 0.0), axis=1, keepdims=True)
    level = whole_square / whole_count
    taps = detection_kernel[...].astype(F32)
    norm = jnp.sum(jnp.sum(taps * taps, axis=1, keepdims=True), axis=0, keepdims=True)
    second = lax.broadcasted_iota(I32, (8, PW), 0) == 1
    numbers[...] = jnp.where(second, 1.0 / jnp.sqrt(1.0 + level * norm), level)
    report = pltpu.make_async_copy(numbers, stats, local.at[4])
    report.start()
    sent(grcv.at[pl.ds(0, GROUP - 1)], 5)
    sent(arcv2.at[pl.ds(0, 7)], 6)
    sent(arcv.at[pl.ds(0, GROUP - 1)], 7)
    sent(db.at[pl.ds(0, dmargin)], 8)
    pltpu.make_async_copy(diffs, diffs, local.at[2]).wait()
    pltpu.make_async_copy(tf, tf, local.at[3]).wait()
    report.wait()


def other_rows(ref, margin, c):
    return ref.at[pl.ds((1 - c) * (ROWS + margin), margin)]


def finish_kernel(difference, filtered, stats, out_difference, out_significance, out_noise, held, sums, numbers, ins, outs):
    loads = [
        pltpu.make_async_copy(stats, numbers, ins.at[0]),
        pltpu.make_async_copy(filtered, sums, ins.at[1]),
        pltpu.make_async_copy(difference, held, ins.at[2]),
    ]
    stores = [
        pltpu.make_async_copy(numbers.at[pl.ds(0, 1)], out_noise, outs.at[0]),
        pltpu.make_async_copy(sums, out_significance, outs.at[1]),
        pltpu.make_async_copy(held, out_difference, outs.at[2]),
    ]
    for load in loads:
        load.start()
    loads[0].wait()
    stores[0].start()
    loads[1].wait()
    sums[...] = sums[...] * numbers[1:2, 0:1]
    stores[1].start()
    loads[2].wait()
    stores[2].start()
    for store in stores:
        store.wait()


def on_device(
    exposure, row_shift, row_fraction, column_shift, column_fraction, piece_width,
    route_tile, route_cell, template, match_kernel, detection_kernel,
):
    vmem = pl.BlockSpec(memory_space=pltpu.VMEM)
    far = pl.BlockSpec(memory_space=pl.ANY)
    wide = template.shape[2]
    margin, dmargin = KS // 2, DK // 2
    difference, filtered, stats = pl.pallas_call(
        kernel,
        out_shape=(
            jax.ShapeDtypeStruct((ROWS, wide), F32),
            jax.ShapeDtypeStruct((ROWS, wide), F32),
            jax.ShapeDtypeStruct((8, PW), F32),
        ),
        in_specs=[far, far, vmem, vmem] + [far] * 7,
        out_specs=(far, far, far),
        scratch_shapes=[
            pltpu.VMEM((ROWS + HALO, NP, PW), F32),
            pltpu.VMEM((HALO, NP, PW), F32),
            pltpu.VMEM((ROWS, CAP, PW), F32),
            pltpu.VMEM((ROWS + 2 * margin, CAP, PW), BF16),
            pltpu.VMEM((ROWS, 1, PW), F32),
            pltpu.VMEM((NP, PW), F32),
            pltpu.VMEM((NP, PW), F32),
            pltpu.VMEM((GROUP, NP, PW), BF16),
            pltpu.VMEM((GROUP, NP, PW), BF16),
            pltpu.VMEM((NX - 1, GROUP, NP, PW), BF16),
            pltpu.VMEM((GROUP * CAP, PW), F32),
            pltpu.VMEM((GROUP, ROWS, PW), BF16),
            pltpu.VMEM((GROUP, ROWS, PW), BF16),
            pltpu.VMEM((NY * CAP, PW), F32),
            pltpu.VMEM((GROUP, ROWS, PW), BF16),
            pltpu.VMEM((GROUP, ROWS, PW), BF16),
            pltpu.VMEM((GROUP, ROWS, PW), F32),
            pltpu.VMEM((48 * 8, PW), F32),
            pltpu.VMEM((48 * 8, PW), F32),
            pltpu.VMEM(((KS + 2) * 2 * PW, PW), BF16),
            pltpu.VMEM(((DK + 2) * 2 * PW, PW), BF16),
            pltpu.VMEM((2, (ROWS // 2 + margin) * CAP, 2 * PW), BF16),
            pltpu.VMEM((2, (ROWS // 2 + dmargin) * CAP, 2 * PW), BF16),
            pltpu.VMEM((ROWS // 2 * CAP, 2 * PW), F32),
            pltpu.VMEM((ROWS, CAP, PW), F32),
            pltpu.VMEM((ROWS, CAP, PW), F32),
            pltpu.VMEM((ROWS + 2 * dmargin, CAP, PW), BF16),
            pltpu.VMEM((1, PW), F32),
            pltpu.VMEM((GROUP, 1, PW), F32),
            pltpu.VMEM((1, PW), F32),
            pltpu.VMEM((8, 1, PW), F32),
            pltpu.VMEM((8, PW), F32),
            pltpu.SemaphoreType.DMA((13,)),
            pltpu.SemaphoreType.DMA((9,)),
            pltpu.SemaphoreType.DMA((17,)),
            pltpu.VMEM((1, ROWS), BF16),
            pltpu.VMEM((1, NP * PW), BF16),
            pltpu.VMEM((1, NP), I32),
            pltpu.VMEM((1, NP), I32),
            pltpu.VMEM((1, NP), I32),
            pltpu.VMEM((KS, KS), BF16),
            pltpu.VMEM((DK, DK), BF16),
        ],
        compiler_params=pltpu.CompilerParams(collective_id=0, has_side_effects=True, vmem_limit_bytes=60 * 1024 * 1024),
        name="warp_match_detect",
    )(
        exposure[0], template[0], row_shift, column_shift, row_fraction, column_fraction,
        piece_width, route_tile, route_cell, match_kernel[0], detection_kernel[0],
    )
    difference, significance, noise = pl.pallas_call(
        finish_kernel,
        out_shape=(
            jax.ShapeDtypeStruct((ROWS, wide), F32),
            jax.ShapeDtypeStruct((ROWS, wide), F32),
            jax.ShapeDtypeStruct((1, PW), F32),
        ),
        in_specs=[far] * 3,
        out_specs=(far, far, far),
        scratch_shapes=[
            pltpu.VMEM((ROWS, wide), F32),
            pltpu.VMEM((ROWS, wide), F32),
            pltpu.VMEM((8, PW), F32),
            pltpu.SemaphoreType.DMA((3,)),
            pltpu.SemaphoreType.DMA((3,)),
        ],
        compiler_params=pltpu.CompilerParams(vmem_limit_bytes=60 * 1024 * 1024),
        name="finish",
    )(difference, filtered, stats)
    return difference[None], significance[None], noise[0, 0]


def solution(mesh):
    finer = Mesh(
        mesh.devices.reshape(NZ, NX, NY, mesh.shape["row"]), ("ccd_0", "ccd_1", "ccd_2", "row")
    )
    placed = (
        P(CCD, "row", None),
        P(CCD),
        P(CCD, "row"),
        P(CCD),
        P(CCD, None),
        P(CCD, None),
        P(CCD, None),
        P(CCD, None),
        P(CCD, "row", None),
        P(CCD, None, None),
        P(CCD, None, None),
    )
    return jax.shard_map(
        on_device,
        mesh=finer,
        in_specs=placed,
        out_specs=(P(CCD, "row", None), P(CCD, "row", None), P()),
        check_vma=False,
    )
```

```python
import functools

import jax
import jax.numpy as jnp
from jax import lax
from jax.experimental import pallas as pl
from jax.experimental.pallas import tpu as pltpu
from jax.sharding import Mesh
from jax.sharding import PartitionSpec as P

PW = 128
HALO = 8
KS = 41
DK = 15
NZ, NX, NY = 8, 4, 4
GROUP = NZ * NY
NP = 16
CAP = 32
ROWS = 24
FR = ROWS // NZ
FL = PW // NY
EARLY = 5
MESH = pl.DeviceIdType.MESH
CCD = ("ccd_0", "ccd_1", "ccd_2")
F32, BF16, I32 = jnp.float32, jnp.bfloat16, jnp.int32


def lanes_of(shape):
    return lax.broadcasted_iota(I32, shape, len(shape) - 1)


def column_of(row, count):
    spread = jnp.broadcast_to(row, (count, count))
    pick = lax.broadcasted_iota(I32, (count, count), 0) == lanes_of((count, count))
    return jnp.sum(jnp.where(pick, spread, 0.0), axis=1, keepdims=True)


def down(x):
    rolled = pltpu.roll(x, 1, 0)
    return jnp.where(lax.broadcasted_iota(I32, x.shape, 0) == 0, 0.0, rolled)


def up(x):
    rolled = pltpu.roll(x, x.shape[0] - 1, 0)
    return jnp.where(lax.broadcasted_iota(I32, x.shape, 0) == x.shape[0] - 1, 0.0, rolled)


def band_bases(kernel_ref, extent, base_lo, base_hi, bands):
    depth = lax.broadcasted_iota(I32, (extent, 2 * PW), 0)
    place = lanes_of((extent, 2 * PW))
    picker = (lax.rem(depth + place, 2 * PW) == 0).astype(F32).astype(BF16)
    turned = jnp.dot(kernel_ref[...], picker, preferred_element_type=F32)
    for s in range(8):
        rolled = pltpu.roll(turned, s, 1) if s else turned
        base_lo[pl.ds(s, extent, stride=8), :] = rolled[:, :PW]
        base_hi[pl.ds(s, extent, stride=8), :] = rolled[:, PW:]
    bands[0:2 * PW, :] = jnp.zeros((2 * PW, PW), BF16)
    bands[(extent + 1) * 2 * PW:(extent + 2) * 2 * PW, :] = jnp.zeros((2 * PW, PW), BF16)


def build_bands(base_lo, base_hi, bands, extent, unroll):
    lane = lanes_of((8, PW))

    def step(a, carry):
        lo = base_lo[pl.ds(pl.multiple_of(a * 8, 8), 8), :]
        hi = base_hi[pl.ds(pl.multiple_of(a * 8, 8), 8), :]
        for pair in range(8):
            near, far = [], []
            for m in (2 * pair, 2 * pair + 1):
                shift = 8 * m
                rlo = pltpu.roll(lo, shift, 1) if shift else lo
                rhi = pltpu.roll(hi, shift, 1) if shift else hi
                near.append(jnp.where(lane >= shift, rlo, rhi))
                far.append(jnp.where(lane >= shift, rhi, rlo))
            for value, start in ((near, 16 * pair), (far, PW + 16 * pair)):
                at = pl.multiple_of((a + 1) * 2 * PW + start, 16)
                bands[pl.ds(at, 16), :] = jnp.concatenate(value, axis=0).astype(BF16)
        return carry

    lax.fori_loop(0, extent, step, 0, unroll=unroll)


def build_windows(rows_ref, start, count, margin, windows, unroll):
    lane = lanes_of((CAP, PW))

    def step(i, carry):
        r = start + i
        shifted = pltpu.roll(rows_ref[r].astype(F32), margin, 1)
        first = jnp.where(lane < margin, down(shifted), shifted)
        second = jnp.where(lane < margin, shifted, up(shifted))
        at = pl.ds(pl.multiple_of(r // 2 * CAP, CAP), CAP)
        windows[r % 2, at, 0:PW] = first.astype(BF16)
        windows[r % 2, at, PW:2 * PW] = second.astype(BF16)
        return carry

    lax.fori_loop(0, count, step, 0, unroll=unroll)


def clear_windows(start, count, windows):
    def step(i, carry):
        r = start + i
        at = pl.ds(pl.multiple_of(r // 2 * CAP, CAP), CAP)
        windows[r % 2, at, :] = jnp.zeros((CAP, 2 * PW), BF16)
        return carry

    lax.fori_loop(0, count, step, 0)


def rows_of(pz):
    return pz * 3 % NZ if isinstance(pz, int) else lax.rem(pz * 3, NZ)


def far_first(i):
    half = (i + 1) // 2
    return lax.rem(NZ // 2 + half * (1 - 2 * (i % 2)) + NZ, NZ)


def banded(windows, bands, per_step, first, last, total):
    half = ROWS // 2 * CAP

    def part(step):
        left = []
        for i in range(per_step):
            at = pl.ds(pl.multiple_of((step * per_step + i) * CAP, CAP), half)
            left += [windows[0, at, :], windows[1, at, :]]
        depth = per_step * 4 * PW
        at = pl.multiple_of(step * depth, depth)
        right = jnp.concatenate([bands[pl.ds(at + 2 * PW, depth), :], bands[pl.ds(at, depth), :]], axis=1)
        return jnp.dot(jnp.concatenate(left, axis=1), right, preferred_element_type=F32)

    if first == 0:
        total[...] = part(0)

    def step(i, carry):
        total[...] += part(i)
        return carry

    lax.fori_loop(max(first, 1), last, step, 0)


def kernel(
    exposure, template, *rest):
    row_shift, column_shift, small, rest = *rest[:2], rest[2:9], rest[9:]
    (difference, significance, stats,
    ext, hx, tf, tb, rfw, cfw, meta, msg, rcv, agb, acc, outg, grcv, held, mfr, mrc, alive,
    base_lo, base_hi, bands, dbands, windows, dwindows, total, matched, diffs, db,
    arsrc, arcv, ar2src, arcv2, numbers, local, sends, recvs,
    row_fraction, column_fraction, piece_width, route_tile, route_cell, match_kernel, detection_kernel) = rest
    z, x, y = (lax.axis_index(a) for a in CCD)
    c = lax.axis_index("row")
    me = z * NY + y

    def zpeer(dz, dy):
        pz = lax.rem(z + dz, NZ)
        py = lax.rem(y + dy, NY)
        return pz, py, {"ccd_0": pz, "ccd_2": py}

    def xpeer(dx, dc=0):
        return {"ccd_1": lax.rem(x + dx, NX), "row": lax.rem(c + dc, 2)}

    partner = {"row": 1 - c}
    near = [(dz, dy) for dz in range(NZ) for dy in range(NY) if dz or dy]
    across = [(dx, dc) for dx in range(NX) for dc in range(2) if dx or dc]

    def send(src, dst, stage, device, slot=None):
        pltpu.make_async_remote_copy(
            src_ref=src, dst_ref=dst, send_sem=sends.at[stage], recv_sem=recvs.at[stage if slot is None else slot],
            device_id=device, device_id_type=MESH,
        ).start()

    def arrived(ref, slot):
        pltpu.make_async_copy(ref, ref, recvs.at[slot]).wait()

    def sent(ref, stage):
        pltpu.make_async_copy(ref, ref, sends.at[stage]).wait()

    barrier = pltpu.get_barrier_semaphore()
    for dz, dy in near:
        pl.semaphore_signal(barrier, inc=1, device_id=zpeer(dz, dy)[2], device_id_type=MESH)
    for dx, dc in across:
        pl.semaphore_signal(barrier, inc=1, device_id=xpeer(dx, dc), device_id_type=MESH)
    held_small = (
        row_fraction, column_fraction, piece_width, route_tile, route_cell, match_kernel, detection_kernel,
    )
    loads = [pltpu.make_async_copy(src, dst, local.at[4 + i]) for i, (src, dst) in enumerate(zip(small, held_small))]
    for load in loads:
        load.start()
    for q in range(CAP):
        pltpu.make_async_copy(template.at[:, pl.ds(q * PW, PW)], tf.at[:, q, :], local.at[1]).start()
    for p in range(NP):
        pltpu.make_async_copy(exposure.at[:, pl.ds(p * PW, PW)], ext.at[pl.ds(0, ROWS), p, :], local.at[0]).start()
    for load in loads:
        load.wait()

    fractions = row_fraction[...].astype(F32)
    for r in range(ROWS):
        rfw[r] = jnp.broadcast_to(fractions[:, r:r + 1], (1, PW))
    columns = column_fraction[...].astype(F32)
    for p in range(NP):
        cfw[p:p + 1, :] = columns[:, p * PW:(p + 1) * PW]
    lane16 = lanes_of((NP, PW))
    width16 = column_of(piece_width[...].astype(F32), NP)
    tile16 = column_of(route_tile[...].astype(F32), NP)
    cell16 = column_of(route_cell[...].astype(F32), NP)
    meta[...] = jnp.where(lane16 == 96, tile16, jnp.where(lane16 == 97, cell16, jnp.where(lane16 == 98, width16, 0.0)))
    margin, dmargin = KS // 2, DK // 2
    pltpu.make_async_copy(tf, tf, local.at[1]).wait()

    def round_template(r, carry):
        tb[margin + r] = tf[r].astype(BF16)
        return carry

    lax.fori_loop(0, ROWS, round_template, 0, unroll=4)
    band_bases(match_kernel, KS, base_lo, base_hi, bands)
    build_bands(base_lo, base_hi, bands, KS, 4)
    clear_windows(c * (ROWS + margin), margin, windows)
    clear_windows(c * (ROWS + dmargin), dmargin, dwindows)
    pltpu.make_async_copy(ext.at[pl.ds(0, ROWS)], ext.at[pl.ds(0, ROWS)], local.at[0]).wait()
    t = jnp.max(row_shift[...].reshape(1, 1))
    s = jnp.max(column_shift[...].reshape(1, 1))
    left_turn = lax.rem(PW - s, PW)
    right_turn = PW - 1 - s
    weight = cfw[...]
    inside = lane16.astype(F32) < width16
    head = meta[...]

    def fragments(group):
        rows = []
        for j in range(FR):
            r = group * FR + j
            w = rfw[r]
            mixed = ((1.0 - w) * ext[r + t] + w * ext[r + t + 1]).astype(BF16).astype(F32)
            leftward = pltpu.roll(mixed, left_turn, 1)
            leftward = jnp.where(lane16 < PW - s, leftward, up(leftward))
            rightward = pltpu.roll(mixed, right_turn, 1)
            rightward = jnp.where(lane16 < PW - 1 - s, rightward, up(rightward))
            warped = (1.0 - weight) * leftward + weight * rightward
            rows.append(jnp.where(inside, warped, 0.0))
        out = []
        for py in range(NY):
            value = head
            for j in range(FR):
                turn = (FL * (j - py)) % PW
                moved = pltpu.roll(rows[j], turn, 1) if turn else rows[j]
                value = jnp.where((lane16 >= FL * j) & (lane16 < FL * (j + 1)), moved, value)
            out.append(value.astype(BF16))
        return out

    def place_fragments(pz):
        for py, value in enumerate(fragments(rows_of(pz))):
            msg[pz * NY + py] = value

    def spread(pz):
        d = lax.rem(pz - z + NZ, NZ)
        dist = d + (NZ - 2 * d) * (d // 5)
        slot = 2 + (dist + 6) // 8 + (dist + 5) // 8
        for dy in range(NY):
            py = lax.rem(y + dy, NY)

            def go():
                send(msg.at[pz * NY + py], rcv.at[me], 2, {"ccd_0": pz, "ccd_2": py}, slot)

            if dy:
                go()
            else:
                pl.when(z != pz)(go)

    for r in range(HALO):
        ext[ROWS + r] = jnp.zeros((NP, PW), F32)
    planes = [rows_of(group) for group in range(NZ)]
    for pz in planes[:EARLY]:
        place_fragments(pz)
    pl.semaphore_wait(barrier, len(near) + len(across))

    pl.when(c == 1)(lambda: send(ext.at[pl.ds(0, HALO)], hx, 0, partner))
    send(tb.at[pl.ds(margin + (1 - c) * (ROWS - margin), margin)], tb.at[pl.ds(c * (ROWS + margin), margin)], 1, partner)
    for pz in planes[:EARLY]:
        spread(pz)
    build_windows(tb, margin, ROWS, margin, windows, 4)

    @pl.when(c == 0)
    def _():
        arrived(hx, 0)
        for r in range(HALO):
            ext[ROWS + r] = hx[r]


    for pz in planes[EARLY:]:
        place_fragments(pz)
        spread(pz)
    rcv[me] = msg[me]

    def forward(slot, distances, count):
        arrived(rcv.at[pl.ds(0, count)], slot)
        for dz in distances:
            at = pl.ds(lax.rem(z + dz, NZ) * NY, NY)
            send(rcv.at[at], agb.at[0, at], 3, xpeer(1), slot=slot + 8)
            send(rcv.at[at], agb.at[2, at], 3, xpeer(3), slot=slot + 11)
            if slot > 2:
                send(rcv.at[at], agb.at[1, at], 3, xpeer(2), slot=16)

    def beside(group, count):
        taken = pl.ds(0, count * NY)
        arrived(agb.at[0, taken], 10 + group)
        arrived(agb.at[2, taken], 13 + group)

    def relay(distances):
        for dz in distances:
            start = lax.rem(z + dz, NZ) * NY
            low, high = pl.ds(start, NY // 2), pl.ds(start + NY // 2, NY // 2)
            send(agb.at[0, low], agb.at[1, low], 3, xpeer(1), slot=16)
            send(agb.at[2, high], agb.at[1, high], 3, xpeer(3), slot=16)

    arrived(other_rows(tb, margin, c), 1)
    build_windows(tb, (1 - c) * (ROWS + margin), margin, margin, windows, 4)
    banded(windows, bands, 3, 0, 5, total)
    forward(2, (0, 1, 7), 11)
    forward(3, (2, 6), 8)
    banded(windows, bands, 3, 5, 7, total)
    forward(4, (3, 5, 4), 12)

    def unpair(q, carry):
        at = pl.ds(pl.multiple_of(q * CAP, CAP), CAP)
        matched[2 * q] = total[at, 0:PW]
        matched[2 * q + 1] = total[at, PW:2 * PW]
        return carry

    lax.fori_loop(0, ROWS // 2, unpair, 0, unroll=2)
    lane24 = lanes_of((ROWS, PW))

    def split(pz):
        for py in range(NY):
            value, last = None, []
            for j in range(FR):
                turn = (FL * (j - py)) % PW
                row = matched[rows_of(pz) * FR + j]
                moved = pltpu.roll(row[:ROWS], turn, 1) if turn else row[:ROWS]
                value = moved if value is None else jnp.where(lane24 >= FL * j, moved, value)
                turn = (FL * (FR - py)) % PW
                last.append(pltpu.roll(row[ROWS:], turn, 1) if turn else row[ROWS:])
            value = jnp.where(lane24 >= FR * FL, jnp.concatenate(last, axis=0), value)
            mfr[pz * NY + py] = value.astype(BF16)

    def follow(i, carry):
        dz = far_first(i)
        pz = lax.rem(z + dz, NZ)
        split(pz)
        for dy in range(NY):
            _, py, device = zpeer(dz, dy)
            send(mfr.at[pz * NY + py], mrc.at[me], 4, device, 5)
        return carry

    lax.fori_loop(0, NZ - 1, follow, 0, unroll=7)
    split(z)
    for dy in range(1, NY):
        _, py, device = zpeer(0, dy)
        send(mfr.at[z * NY + py], mrc.at[me], 4, device, 5)
    mrc[me] = mfr[me]

    def codes(block):
        picks = (lanes_of((8, PW)) == lax.broadcasted_iota(I32, (8, PW), 0) + 96).astype(F32).astype(BF16)
        rows = lax.dot_general(picks, block, (((1,), (1,)), ((), ())), preferred_element_type=F32)
        tile = rows[0:1, :].astype(I32)
        cell = rows[1:2, :].astype(I32)
        tz, tx, ty = tile // (NX * NY), (tile // NY) % NX, tile % NY
        return jnp.where(tx == x, (tz * NY + ty) * CAP + cell, -1)

    chunk = NY * CAP
    chunk_rows = lax.broadcasted_iota(I32, (chunk, GROUP * NP), 0)

    def chosen(code, block, pz):
        hot = (chunk_rows == code - pz * chunk).astype(F32).astype(BF16)
        return jnp.dot(hot, block, preferred_element_type=F32)

    def flat(ref):
        return ref[...].reshape(GROUP * NP, PW)

    def add_block(block, first):
        code = codes(block)

        def step(pz, carry):
            at = pl.ds(pl.multiple_of(pz * chunk, chunk), chunk)
            value = chosen(code, block, pz)
            acc[at, :] = value if first else acc[at, :] + value
            return carry

        lax.fori_loop(0, NZ, step, 0, unroll=8)

    add_block(flat(rcv), True)
    beside(0, 3)
    relay((0, 1, 7))
    beside(1, 2)
    beside(2, 3)
    add_block(flat(agb.at[2]), False)
    add_block(flat(agb.at[0]), False)
    arrived(agb.at[1], 16)
    block = flat(agb.at[1])
    code = codes(block)
    lane8 = lanes_of((8, PW))

    def finish(pz):
        at = pl.ds(pl.multiple_of(pz * chunk, chunk), chunk)
        value = acc[at, :] + chosen(code, block, pz)
        acc[at, :] = value
        for py in range(NY):
            tile = value[py * CAP:(py + 1) * CAP]
            rows = []
            for j in range(FR):
                turn = (FL * (FR - j)) % PW
                rows.append(jnp.where(lane8 >= FR * FL, pltpu.roll(tile[ROWS:], turn, 1), tile[8 * j:8 * j + 8]))
            outg[pz * NY + py] = jnp.concatenate(rows, axis=0).astype(BF16)
        return value

    def deliver(i, carry):
        dz = far_first(i)
        pz = lax.rem(z + dz, NZ)
        finish(pz)
        for dy in range(NY):
            _, py, device = zpeer(dz, dy)
            send(outg.at[pz * NY + py], grcv.at[me], 5, device, 6)
        return carry

    lax.fori_loop(0, NZ - 1, deliver, 0, unroll=7)
    held[...] = finish(z)
    for dy in range(1, NY):
        _, py, device = zpeer(0, dy)
        send(outg.at[z * NY + py], grcv.at[me], 5, device, 6)
    grcv[me] = outg[me]

    lane32 = lanes_of((CAP, PW))
    own = held[pl.ds(pl.multiple_of(y * CAP, CAP), CAP), :]
    width32 = jnp.sum(jnp.where(lane32 == 98, own, 0.0), axis=1, keepdims=True)
    live = lane32.astype(F32) < width32
    live_count = ROWS * jnp.sum(width32, axis=0, keepdims=True)
    place = (lax.rem(lane24, FL) + FL * y).astype(F32)

    def mark_live(k, carry):
        value = acc[pl.ds(pl.multiple_of(k * CAP, CAP), CAP), :]
        width = jnp.sum(jnp.where(lane32 == 98, value, 0.0), axis=1, keepdims=True)
        last = jnp.concatenate([width[ROWS:]] * FR, axis=0)
        width = jnp.where(lane24 < FR * FL, width[:ROWS], last)
        alive[k] = jnp.where(place < width, 1.0, 0.0)
        return carry

    lax.fori_loop(0, GROUP, mark_live, 0, unroll=8)
    arrived(mrc.at[pl.ds(0, GROUP - 1)], 5)

    def square(k, squares):
        value = (outg[k].astype(F32) - mrc[k].astype(F32)) * alive[k]
        return squares + value * value

    squares = lax.fori_loop(0, GROUP, square, jnp.zeros((ROWS, PW), F32), unroll=8)
    square_sum = jnp.sum(jnp.sum(squares, axis=1, keepdims=True), axis=0, keepdims=True)
    lane1 = lanes_of((1, PW))
    arsrc[...] = jnp.where(lane1 == 0, square_sum, jnp.where(lane1 == 1, live_count, 0.0))
    for dx, dc in across:
        send(arsrc, arcv2.at[x * 2 + c], 6, xpeer(dx, dc), 7)
    arcv2[x * 2 + c] = arsrc[...]
    band_bases(detection_kernel, DK, base_lo, base_hi, dbands)
    build_bands(base_lo, base_hi, dbands, DK, 5)
    sent(rcv.at[pl.ds(0, GROUP - 1)], 2)
    sent(agb, 3)
    pl.when(c == 1)(lambda: sent(hx, 0))
    sent(tb.at[pl.ds(0, margin)], 1)
    sent(mrc.at[pl.ds(0, GROUP - 1)], 4)
    arrived(arcv2.at[pl.ds(0, 7)], 7)
    ar2src[...] = jnp.sum(arcv2[...], axis=0)
    for dz, dy in near:
        send(ar2src, arcv.at[me], 7, zpeer(dz, dy)[2], 8)
    arcv[me] = ar2src[...]
    arrived(grcv.at[pl.ds(0, GROUP - 1)], 6)

    def subtract(pz, carry):
        parts = [grcv[pz * NY + py].astype(F32) for py in range(NY)]
        for j in range(FR):
            science = None
            for py in range(NY):
                turn = (FL * (py - j)) % PW
                moved = pltpu.roll(parts[py], turn, 1) if turn else parts[py]
                turn = (FL * (py - FR)) % PW
                rest = parts[py][8 * j:8 * j + 8]
                rest = pltpu.roll(rest, turn, 1) if turn else rest
                moved = jnp.concatenate([moved, rest], axis=0)
                science = moved if science is None else jnp.where(lane32 >= FL * py, moved, science)
            r = rows_of(pz) * FR + j
            value = jnp.where(live, science - matched[r], 0.0)
            diffs[r] = value
            db[dmargin + r] = value.astype(BF16)
        return carry

    lax.fori_loop(0, NZ, subtract, 0, unroll=4)
    send(db.at[pl.ds(dmargin + (1 - c) * (ROWS - dmargin), dmargin)], db.at[pl.ds(c * (ROWS + dmargin), dmargin)], 8, partner, 9)
    for q in range(CAP):
        pltpu.make_async_copy(diffs.at[:, q, :], difference.at[:, pl.ds(q * PW, PW)], local.at[2]).start()
    build_windows(db, dmargin, ROWS, dmargin, dwindows, 4)

    arrived(other_rows(db, dmargin, c), 9)
    build_windows(db, (1 - c) * (ROWS + dmargin), dmargin, dmargin, dwindows, 7)
    banded(dwindows, dbands, 4, 0, (DK + 1) // 8, total)

    def unpair_filtered(q, carry):
        at = pl.ds(pl.multiple_of(q * CAP, CAP), CAP)
        tf[2 * q] = total[at, 0:PW]
        tf[2 * q + 1] = total[at, PW:2 * PW]
        return carry

    lax.fori_loop(0, ROWS // 2, unpair_filtered, 0, unroll=6)
    for q in range(CAP):
        pltpu.make_async_copy(tf.at[:, q, :], significance.at[:, pl.ds(q * PW, PW)], local.at[3]).start()
    arrived(arcv.at[pl.ds(0, GROUP - 1)], 8)
    sums = jnp.sum(arcv[...], axis=0)
    whole_square = jnp.sum(jnp.where(lane1 == 0, sums, 0.0), axis=1, keepdims=True)
    whole_count = jnp.sum(jnp.where(lane1 == 1, sums, 0.0), axis=1, keepdims=True)
    level = whole_square / whole_count
    taps = detection_kernel[...].astype(F32)
    norm = jnp.sum(jnp.sum(taps * taps, axis=1, keepdims=True), axis=0, keepdims=True)
    second = lax.broadcasted_iota(I32, (8, PW), 0) == 1
    numbers[...] = jnp.where(second, 1.0 / jnp.sqrt(1.0 + level * norm), level)
    report = pltpu.make_async_copy(numbers, stats, local.at[4])
    report.start()
    sent(grcv.at[pl.ds(0, GROUP - 1)], 5)
    sent(arcv2.at[pl.ds(0, 7)], 6)
    sent(arcv.at[pl.ds(0, GROUP - 1)], 7)
    sent(db.at[pl.ds(0, dmargin)], 8)
    pltpu.make_async_copy(diffs, diffs, local.at[2]).wait()
    pltpu.make_async_copy(tf, tf, local.at[3]).wait()
    report.wait()


def other_rows(ref, margin, c):
    return ref.at[pl.ds((1 - c) * (ROWS + margin), margin)]


def finish_kernel(difference, filtered, stats, out_difference, out_significance, out_noise, held, sums, numbers, ins, outs):
    loads = [
        pltpu.make_async_copy(stats, numbers, ins.at[0]),
        pltpu.make_async_copy(filtered, sums, ins.at[1]),
        pltpu.make_async_copy(difference, held, ins.at[2]),
    ]
    stores = [
        pltpu.make_async_copy(numbers.at[pl.ds(0, 1)], out_noise, outs.at[0]),
        pltpu.make_async_copy(sums, out_significance, outs.at[1]),
        pltpu.make_async_copy(held, out_difference, outs.at[2]),
    ]
    for load in loads:
        load.start()
    loads[0].wait()
    stores[0].start()
    loads[1].wait()
    sums[...] = sums[...] * numbers[1:2, 0:1]
    stores[1].start()
    loads[2].wait()
    stores[2].start()
    for store in stores:
        store.wait()


def on_device(
    exposure, row_shift, row_fraction, column_shift, column_fraction, piece_width,
    route_tile, route_cell, template, match_kernel, detection_kernel,
):
    vmem = pl.BlockSpec(memory_space=pltpu.VMEM)
    far = pl.BlockSpec(memory_space=pl.ANY)
    wide = template.shape[2]
    margin, dmargin = KS // 2, DK // 2
    difference, filtered, stats = pl.pallas_call(
        kernel,
        out_shape=(
            jax.ShapeDtypeStruct((ROWS, wide), F32),
            jax.ShapeDtypeStruct((ROWS, wide), F32),
            jax.ShapeDtypeStruct((8, PW), F32),
        ),
        in_specs=[far, far, vmem, vmem] + [far] * 7,
        out_specs=(far, far, far),
        scratch_shapes=[
            pltpu.VMEM((ROWS + HALO, NP, PW), F32),
            pltpu.VMEM((HALO, NP, PW), F32),
            pltpu.VMEM((ROWS, CAP, PW), F32),
            pltpu.VMEM((ROWS + 2 * margin, CAP, PW), BF16),
            pltpu.VMEM((ROWS, 1, PW), F32),
            pltpu.VMEM((NP, PW), F32),
            pltpu.VMEM((NP, PW), F32),
            pltpu.VMEM((GROUP, NP, PW), BF16),
            pltpu.VMEM((GROUP, NP, PW), BF16),
            pltpu.VMEM((NX - 1, GROUP, NP, PW), BF16),
            pltpu.VMEM((GROUP * CAP, PW), F32),
            pltpu.VMEM((GROUP, ROWS, PW), BF16),
            pltpu.VMEM((GROUP, ROWS, PW), BF16),
            pltpu.VMEM((NY * CAP, PW), F32),
            pltpu.VMEM((GROUP, ROWS, PW), BF16),
            pltpu.VMEM((GROUP, ROWS, PW), BF16),
            pltpu.VMEM((GROUP, ROWS, PW), F32),
            pltpu.VMEM((48 * 8, PW), F32),
            pltpu.VMEM((48 * 8, PW), F32),
            pltpu.VMEM(((KS + 2) * 2 * PW, PW), BF16),
            pltpu.VMEM(((DK + 2) * 2 * PW, PW), BF16),
            pltpu.VMEM((2, (ROWS // 2 + margin) * CAP, 2 * PW), BF16),
            pltpu.VMEM((2, (ROWS // 2 + dmargin) * CAP, 2 * PW), BF16),
            pltpu.VMEM((ROWS // 2 * CAP, 2 * PW), F32),
            pltpu.VMEM((ROWS, CAP, PW), F32),
            pltpu.VMEM((ROWS, CAP, PW), F32),
            pltpu.VMEM((ROWS + 2 * dmargin, CAP, PW), BF16),
            pltpu.VMEM((1, PW), F32),
            pltpu.VMEM((GROUP, 1, PW), F32),
            pltpu.VMEM((1, PW), F32),
            pltpu.VMEM((8, 1, PW), F32),
            pltpu.VMEM((8, PW), F32),
            pltpu.SemaphoreType.DMA((13,)),
            pltpu.SemaphoreType.DMA((9,)),
            pltpu.SemaphoreType.DMA((17,)),
            pltpu.VMEM((1, ROWS), BF16),
            pltpu.VMEM((1, NP * PW), BF16),
            pltpu.VMEM((1, NP), I32),
            pltpu.VMEM((1, NP), I32),
            pltpu.VMEM((1, NP), I32),
            pltpu.VMEM((KS, KS), BF16),
            pltpu.VMEM((DK, DK), BF16),
        ],
        compiler_params=pltpu.CompilerParams(collective_id=0, has_side_effects=True, vmem_limit_bytes=60 * 1024 * 1024),
        name="warp_match_detect",
    )(
        exposure[0], template[0], row_shift, column_shift, row_fraction, column_fraction,
        piece_width, route_tile, route_cell, match_kernel[0], detection_kernel[0],
    )
    difference, significance, noise = pl.pallas_call(
        finish_kernel,
        out_shape=(
            jax.ShapeDtypeStruct((ROWS, wide), F32),
            jax.ShapeDtypeStruct((ROWS, wide), F32),
            jax.ShapeDtypeStruct((1, PW), F32),
        ),
        in_specs=[far] * 3,
        out_specs=(far, far, far),
        scratch_shapes=[
            pltpu.VMEM((ROWS, wide), F32),
            pltpu.VMEM((ROWS, wide), F32),
            pltpu.VMEM((8, PW), F32),
            pltpu.SemaphoreType.DMA((3,)),
            pltpu.SemaphoreType.DMA((3,)),
        ],
        compiler_params=pltpu.CompilerParams(vmem_limit_bytes=60 * 1024 * 1024),
        name="finish",
    )(difference, filtered, stats)
    return difference[None], significance[None], noise[0, 0]


def solution(mesh):
    finer = Mesh(
        mesh.devices.reshape(NZ, NX, NY, mesh.shape["row"]), ("ccd_0", "ccd_1", "ccd_2", "row")
    )
    placed = (
        P(CCD, "row", None),
        P(CCD),
        P(CCD, "row"),
        P(CCD),
        P(CCD, None),
        P(CCD, None),
        P(CCD, None),
        P(CCD, None),
        P(CCD, "row", None),
        P(CCD, None, None),
        P(CCD, None, None),
    )
    return jax.shard_map(
        on_device,
        mesh=finer,
        in_specs=placed,
        out_specs=(P(CCD, "row", None), P(CCD, "row", None), P()),
        check_vma=False,
    )
```

```python
import functools

import jax
import jax.numpy as jnp
from jax import lax
from jax.experimental import pallas as pl
from jax.experimental.pallas import tpu as pltpu
from jax.sharding import Mesh
from jax.sharding import PartitionSpec as P

PW = 128
HALO = 8
KS = 41
DK = 15
NZ, NX, NY = 8, 4, 4
GROUP = NZ * NY
NP = 16
CAP = 32
ROWS = 24
FR = ROWS // NZ
FL = PW // NY
EARLY = 5
MESH = pl.DeviceIdType.MESH
CCD = ("ccd_0", "ccd_1", "ccd_2")
F32, BF16, I32 = jnp.float32, jnp.bfloat16, jnp.int32


def lanes_of(shape):
    return lax.broadcasted_iota(I32, shape, len(shape) - 1)


def column_of(row, count):
    spread = jnp.broadcast_to(row, (count, count))
    pick = lax.broadcasted_iota(I32, (count, count), 0) == lanes_of((count, count))
    return jnp.sum(jnp.where(pick, spread, 0.0), axis=1, keepdims=True)


def down(x):
    rolled = pltpu.roll(x, 1, 0)
    return jnp.where(lax.broadcasted_iota(I32, x.shape, 0) == 0, 0.0, rolled)


def up(x):
    rolled = pltpu.roll(x, x.shape[0] - 1, 0)
    return jnp.where(lax.broadcasted_iota(I32, x.shape, 0) == x.shape[0] - 1, 0.0, rolled)


def band_bases(kernel_ref, extent, base_lo, base_hi, bands):
    depth = lax.broadcasted_iota(I32, (extent, 2 * PW), 0)
    place = lanes_of((extent, 2 * PW))
    picker = (lax.rem(depth + place, 2 * PW) == 0).astype(F32).astype(BF16)
    turned = jnp.dot(kernel_ref[...], picker, preferred_element_type=F32)
    for s in range(8):
        rolled = pltpu.roll(turned, s, 1) if s else turned
        base_lo[pl.ds(s, extent, stride=8), :] = rolled[:, :PW]
        base_hi[pl.ds(s, extent, stride=8), :] = rolled[:, PW:]
    bands[0:2 * PW, :] = jnp.zeros((2 * PW, PW), BF16)
    bands[(extent + 1) * 2 * PW:(extent + 2) * 2 * PW, :] = jnp.zeros((2 * PW, PW), BF16)


def build_bands(base_lo, base_hi, bands, extent, unroll):
    lane = lanes_of((8, PW))

    def step(a, carry):
        lo = base_lo[pl.ds(pl.multiple_of(a * 8, 8), 8), :]
        hi = base_hi[pl.ds(pl.multiple_of(a * 8, 8), 8), :]
        for pair in range(8):
            near, far = [], []
            for m in (2 * pair, 2 * pair + 1):
                shift = 8 * m
                rlo = pltpu.roll(lo, shift, 1) if shift else lo
                rhi = pltpu.roll(hi, shift, 1) if shift else hi
                near.append(jnp.where(lane >= shift, rlo, rhi))
                far.append(jnp.where(lane >= shift, rhi, rlo))
            for value, start in ((near, 16 * pair), (far, PW + 16 * pair)):
                at = pl.multiple_of((a + 1) * 2 * PW + start, 16)
                bands[pl.ds(at, 16), :] = jnp.concatenate(value, axis=0).astype(BF16)
        return carry

    lax.fori_loop(0, extent, step, 0, unroll=unroll)


def build_windows(rows_ref, start, count, margin, windows, unroll):
    lane = lanes_of((CAP, PW))

    def step(i, carry):
        r = start + i
        shifted = pltpu.roll(rows_ref[r].astype(F32), margin, 1)
        first = jnp.where(lane < margin, down(shifted), shifted)
        second = jnp.where(lane < margin, shifted, up(shifted))
        at = pl.ds(pl.multiple_of(r // 2 * CAP, CAP), CAP)
        windows[r % 2, at, 0:PW] = first.astype(BF16)
        windows[r % 2, at, PW:2 * PW] = second.astype(BF16)
        return carry

    lax.fori_loop(0, count, step, 0, unroll=unroll)


def clear_windows(start, count, windows):
    def step(i, carry):
        r = start + i
        at = pl.ds(pl.multiple_of(r // 2 * CAP, CAP), CAP)
        windows[r % 2, at, :] = jnp.zeros((CAP, 2 * PW), BF16)
        return carry

    lax.fori_loop(0, count, step, 0)


def rows_of(pz):
    return pz * 3 % NZ if isinstance(pz, int) else lax.rem(pz * 3, NZ)


def far_first(i):
    half = (i + 1) // 2
    return lax.rem(NZ // 2 + half * (1 - 2 * (i % 2)) + NZ, NZ)


def banded(windows, bands, per_step, first, last, total):
    half = ROWS // 2 * CAP

    def part(step):
        left = []
        for i in range(per_step):
            at = pl.ds(pl.multiple_of((step * per_step + i) * CAP, CAP), half)
            left += [windows[0, at, :], windows[1, at, :]]
        depth = per_step * 4 * PW
        at = pl.multiple_of(step * depth, depth)
        right = jnp.concatenate([bands[pl.ds(at + 2 * PW, depth), :], bands[pl.ds(at, depth), :]], axis=1)
        return jnp.dot(jnp.concatenate(left, axis=1), right, preferred_element_type=F32)

    if first == 0:
        total[...] = part(0)

    def step(i, carry):
        total[...] += part(i)
        return carry

    lax.fori_loop(max(first, 1), last, step, 0)


def kernel(
    exposure, template, *rest):
    row_shift, column_shift, small, rest = *rest[:2], rest[2:9], rest[9:]
    (difference, significance, stats,
    ext, hx, tf, tb, rfw, cfw, meta, msg, rcv, agb, acc, outg, grcv, held, mfr, mrc, alive,
    base_lo, base_hi, bands, dbands, windows, dwindows, total, matched, diffs, db,
    arsrc, arcv, ar2src, arcv2, numbers, local, sends, recvs,
    row_fraction, column_fraction, piece_width, route_tile, route_cell, match_kernel, detection_kernel) = rest
    z, x, y = (lax.axis_index(a) for a in CCD)
    c = lax.axis_index("row")
    me = z * NY + y

    def zpeer(dz, dy):
        pz = lax.rem(z + dz, NZ)
        py = lax.rem(y + dy, NY)
        return pz, py, {"ccd_0": pz, "ccd_2": py}

    def xpeer(dx, dc=0):
        return {"ccd_1": lax.rem(x + dx, NX), "row": lax.rem(c + dc, 2)}

    partner = {"row": 1 - c}
    near = [(dz, dy) for dz in range(NZ) for dy in range(NY) if dz or dy]
    across = [(dx, dc) for dx in range(NX) for dc in range(2) if dx or dc]

    def send(src, dst, stage, device, slot=None):
        pltpu.make_async_remote_copy(
            src_ref=src, dst_ref=dst, send_sem=sends.at[stage], recv_sem=recvs.at[stage if slot is None else slot],
            device_id=device, device_id_type=MESH,
        ).start()

    def arrived(ref, slot):
        pltpu.make_async_copy(ref, ref, recvs.at[slot]).wait()

    def sent(ref, stage):
        pltpu.make_async_copy(ref, ref, sends.at[stage]).wait()

    barrier = pltpu.get_barrier_semaphore()
    for dz, dy in near:
        pl.semaphore_signal(barrier, inc=1, device_id=zpeer(dz, dy)[2], device_id_type=MESH)
    for dx, dc in across:
        pl.semaphore_signal(barrier, inc=1, device_id=xpeer(dx, dc), device_id_type=MESH)
    held_small = (
        row_fraction, column_fraction, piece_width, route_tile, route_cell, match_kernel, detection_kernel,
    )
    loads = [pltpu.make_async_copy(src, dst, local.at[4 + i]) for i, (src, dst) in enumerate(zip(small, held_small))]
    for load in loads:
        load.start()
    for q in range(CAP):
        pltpu.make_async_copy(template.at[:, pl.ds(q * PW, PW)], tf.at[:, q, :], local.at[1]).start()
    for p in range(NP):
        pltpu.make_async_copy(exposure.at[:, pl.ds(p * PW, PW)], ext.at[pl.ds(0, ROWS), p, :], local.at[0]).start()
    for load in loads:
        load.wait()

    fractions = row_fraction[...].astype(F32)
    for r in range(ROWS):
        rfw[r] = jnp.broadcast_to(fractions[:, r:r + 1], (1, PW))
    columns = column_fraction[...].astype(F32)
    for p in range(NP):
        cfw[p:p + 1, :] = columns[:, p * PW:(p + 1) * PW]
    lane16 = lanes_of((NP, PW))
    width16 = column_of(piece_width[...].astype(F32), NP)
    tile16 = column_of(route_tile[...].astype(F32), NP)
    cell16 = column_of(route_cell[...].astype(F32), NP)
    meta[...] = jnp.where(lane16 == 96, tile16, jnp.where(lane16 == 97, cell16, jnp.where(lane16 == 98, width16, 0.0)))
    margin, dmargin = KS // 2, DK // 2
    pltpu.make_async_copy(tf, tf, local.at[1]).wait()

    def round_template(r, carry):
        tb[margin + r] = tf[r].astype(BF16)
        return carry

    lax.fori_loop(0, ROWS, round_template, 0, unroll=4)
    band_bases(match_kernel, KS, base_lo, base_hi, bands)
    build_bands(base_lo, base_hi, bands, KS, 4)
    clear_windows(c * (ROWS + margin), margin, windows)
    clear_windows(c * (ROWS + dmargin), dmargin, dwindows)
    pltpu.make_async_copy(ext.at[pl.ds(0, ROWS)], ext.at[pl.ds(0, ROWS)], local.at[0]).wait()
    t = jnp.max(row_shift[...].reshape(1, 1))
    s = jnp.max(column_shift[...].reshape(1, 1))
    left_turn = lax.rem(PW - s, PW)
    right_turn = PW - 1 - s
    weight = cfw[...]
    inside = lane16.astype(F32) < width16
    head = meta[...]

    def fragments(group):
        rows = []
        for j in range(FR):
            r = group * FR + j
            w = rfw[r]
            mixed = ((1.0 - w) * ext[r + t] + w * ext[r + t + 1]).astype(BF16).astype(F32)
            leftward = pltpu.roll(mixed, left_turn, 1)
            leftward = jnp.where(lane16 < PW - s, leftward, up(leftward))
            rightward = pltpu.roll(mixed, right_turn, 1)
            rightward = jnp.where(lane16 < PW - 1 - s, rightward, up(rightward))
            warped = (1.0 - weight) * leftward + weight * rightward
            rows.append(jnp.where(inside, warped, 0.0))
        out = []
        for py in range(NY):
            value = head
            for j in range(FR):
                turn = (FL * (j - py)) % PW
                moved = pltpu.roll(rows[j], turn, 1) if turn else rows[j]
                value = jnp.where((lane16 >= FL * j) & (lane16 < FL * (j + 1)), moved, value)
            out.append(value.astype(BF16))
        return out

    def place_fragments(pz):
        for py, value in enumerate(fragments(rows_of(pz))):
            msg[pz * NY + py] = value

    def spread(pz):
        d = lax.rem(pz - z + NZ, NZ)
        dist = d + (NZ - 2 * d) * (d // 5)
        slot = 2 + (dist + 6) // 8 + (dist + 5) // 8
        for dy in range(NY):
            py = lax.rem(y + dy, NY)

            def go():
                send(msg.at[pz * NY + py], rcv.at[me], 2, {"ccd_0": pz, "ccd_2": py}, slot)

            if dy:
                go()
            else:
                pl.when(z != pz)(go)

    for r in range(HALO):
        ext[ROWS + r] = jnp.zeros((NP, PW), F32)
    planes = [rows_of(group) for group in range(NZ)]
    for pz in planes[:EARLY]:
        place_fragments(pz)
    pl.semaphore_wait(barrier, len(near) + len(across))

    pl.when(c == 1)(lambda: send(ext.at[pl.ds(0, HALO)], hx, 0, partner))
    send(tb.at[pl.ds(margin + (1 - c) * (ROWS - margin), margin)], tb.at[pl.ds(c * (ROWS + margin), margin)], 1, partner)
    for pz in planes[:EARLY]:
        spread(pz)
    build_windows(tb, margin, ROWS, margin, windows, 4)

    @pl.when(c == 0)
    def _():
        arrived(hx, 0)
        for r in range(HALO):
            ext[ROWS + r] = hx[r]


    for pz in planes[EARLY:]:
        place_fragments(pz)
        spread(pz)
    rcv[me] = msg[me]

    def forward(slot, distances, count):
        arrived(rcv.at[pl.ds(0, count)], slot)
        for dz in distances:
            at = pl.ds(lax.rem(z + dz, NZ) * NY, NY)
            send(rcv.at[at], agb.at[0, at], 3, xpeer(1), slot=slot + 8)
            send(rcv.at[at], agb.at[2, at], 3, xpeer(3), slot=slot + 11)
            if slot > 2:
                send(rcv.at[at], agb.at[1, at], 3, xpeer(2), slot=16)

    def beside(group, count):
        taken = pl.ds(0, count * NY)
        arrived(agb.at[0, taken], 10 + group)
        arrived(agb.at[2, taken], 13 + group)

    def relay(distances):
        for dz in distances:
            start = lax.rem(z + dz, NZ) * NY
            low, high = pl.ds(start, NY // 2), pl.ds(start + NY // 2, NY // 2)
            send(agb.at[0, low], agb.at[1, low], 3, xpeer(1), slot=16)
            send(agb.at[2, high], agb.at[1, high], 3, xpeer(3), slot=16)

    arrived(other_rows(tb, margin, c), 1)
    build_windows(tb, (1 - c) * (ROWS + margin), margin, margin, windows, 4)
    banded(windows, bands, 3, 0, 5, total)
    forward(2, (0, 1, 7), 11)
    forward(3, (2, 6), 8)
    banded(windows, bands, 3, 5, 7, total)
    forward(4, (3, 5, 4), 12)

    def unpair(q, carry):
        at = pl.ds(pl.multiple_of(q * CAP, CAP), CAP)
        matched[2 * q] = total[at, 0:PW]
        matched[2 * q + 1] = total[at, PW:2 * PW]
        return carry

    lax.fori_loop(0, ROWS // 2, unpair, 0, unroll=2)
    lane24 = lanes_of((ROWS, PW))

    def split(pz):
        for py in range(NY):
            value, last = None, []
            for j in range(FR):
                turn = (FL * (j - py)) % PW
                row = matched[rows_of(pz) * FR + j]
                moved = pltpu.roll(row[:ROWS], turn, 1) if turn else row[:ROWS]
                value = moved if value is None else jnp.where(lane24 >= FL * j, moved, value)
                turn = (FL * (FR - py)) % PW
                last.append(pltpu.roll(row[ROWS:], turn, 1) if turn else row[ROWS:])
            value = jnp.where(lane24 >= FR * FL, jnp.concatenate(last, axis=0), value)
            mfr[pz * NY + py] = value.astype(BF16)

    def follow(i, carry):
        dz = far_first(i)
        pz = lax.rem(z + dz, NZ)
        split(pz)
        for dy in range(NY):
            _, py, device = zpeer(dz, dy)
            send(mfr.at[pz * NY + py], mrc.at[me], 4, device, 5)
        return carry

    lax.fori_loop(0, NZ - 1, follow, 0, unroll=7)
    split(z)
    for dy in range(1, NY):
        _, py, device = zpeer(0, dy)
        send(mfr.at[z * NY + py], mrc.at[me], 4, device, 5)
    mrc[me] = mfr[me]

    def codes(block):
        picks = (lanes_of((8, PW)) == lax.broadcasted_iota(I32, (8, PW), 0) + 96).astype(F32).astype(BF16)
        rows = lax.dot_general(picks, block, (((1,), (1,)), ((), ())), preferred_element_type=F32)
        tile = rows[0:1, :].astype(I32)
        cell = rows[1:2, :].astype(I32)
        tz, tx, ty = tile // (NX * NY), (tile // NY) % NX, tile % NY
        return jnp.where(tx == x, (tz * NY + ty) * CAP + cell, -1)

    chunk = NY * CAP
    chunk_rows = lax.broadcasted_iota(I32, (chunk, GROUP * NP), 0)

    def chosen(code, block, pz):
        hot = (chunk_rows == code - pz * chunk).astype(F32).astype(BF16)
        return jnp.dot(hot, block, preferred_element_type=F32)

    def flat(ref):
        return ref[...].reshape(GROUP * NP, PW)

    def add_block(block, first):
        code = codes(block)

        def step(pz, carry):
            at = pl.ds(pl.multiple_of(pz * chunk, chunk), chunk)
            value = chosen(code, block, pz)
            acc[at, :] = value if first else acc[at, :] + value
            return carry

        lax.fori_loop(0, NZ, step, 0, unroll=8)

    add_block(flat(rcv), True)
    beside(0, 3)
    relay((0, 1, 7))
    beside(1, 2)
    beside(2, 3)
    add_block(flat(agb.at[2]), False)
    add_block(flat(agb.at[0]), False)
    arrived(agb.at[1], 16)
    block = flat(agb.at[1])
    code = codes(block)
    lane8 = lanes_of((8, PW))

    def finish(pz):
        at = pl.ds(pl.multiple_of(pz * chunk, chunk), chunk)
        value = acc[at, :] + chosen(code, block, pz)
        acc[at, :] = value
        for py in range(NY):
            tile = value[py * CAP:(py + 1) * CAP]
            rows = []
            for j in range(FR):
                turn = (FL * (FR - j)) % PW
                rows.append(jnp.where(lane8 >= FR * FL, pltpu.roll(tile[ROWS:], turn, 1), tile[8 * j:8 * j + 8]))
            outg[pz * NY + py] = jnp.concatenate(rows, axis=0).astype(BF16)
        return value

    def deliver(i, carry):
        dz = far_first(i)
        pz = lax.rem(z + dz, NZ)
        finish(pz)
        for dy in range(NY):
            _, py, device = zpeer(dz, dy)
            send(outg.at[pz * NY + py], grcv.at[me], 5, device, 6)
        return carry

    lax.fori_loop(0, NZ - 1, deliver, 0, unroll=7)
    held[...] = finish(z)
    for dy in range(1, NY):
        _, py, device = zpeer(0, dy)
        send(outg.at[z * NY + py], grcv.at[me], 5, device, 6)
    grcv[me] = outg[me]

    lane32 = lanes_of((CAP, PW))
    own = held[pl.ds(pl.multiple_of(y * CAP, CAP), CAP), :]
    width32 = jnp.sum(jnp.where(lane32 == 98, own, 0.0), axis=1, keepdims=True)
    live = lane32.astype(F32) < width32
    live_count = ROWS * jnp.sum(width32, axis=0, keepdims=True)
    place = (lax.rem(lane24, FL) + FL * y).astype(F32)

    spot = (lax.broadcasted_iota(I32, (PW, PW), 0) == 98).astype(F32).astype(BF16)

    def mark_live(pz, carry):
        value = acc[pl.ds(pl.multiple_of(pz * chunk, chunk), chunk), :].astype(BF16)
        wide = jnp.dot(value, spot, preferred_element_type=F32)
        for py in range(NY):
            width = wide[py * CAP:(py + 1) * CAP]
            last = jnp.concatenate([width[ROWS:]] * FR, axis=0)
            width = jnp.where(lane24 < FR * FL, width[:ROWS], last)
            alive[pz * NY + py] = jnp.where(place < width, 1.0, 0.0)
        return carry

    lax.fori_loop(0, NZ, mark_live, 0, unroll=4)
    arrived(mrc.at[pl.ds(0, GROUP - 1)], 5)

    def square(k, squares):
        value = (outg[k].astype(F32) - mrc[k].astype(F32)) * alive[k]
        return squares + value * value

    squares = lax.fori_loop(0, GROUP, square, jnp.zeros((ROWS, PW), F32), unroll=8)
    square_sum = jnp.sum(jnp.sum(squares, axis=1, keepdims=True), axis=0, keepdims=True)
    lane1 = lanes_of((1, PW))
    arsrc[...] = jnp.where(lane1 == 0, square_sum, jnp.where(lane1 == 1, live_count, 0.0))
    for dx, dc in across:
        send(arsrc, arcv2.at[x * 2 + c], 6, xpeer(dx, dc), 7)
    arcv2[x * 2 + c] = arsrc[...]
    band_bases(detection_kernel, DK, base_lo, base_hi, dbands)
    build_bands(base_lo, base_hi, dbands, DK, 5)
    sent(rcv.at[pl.ds(0, GROUP - 1)], 2)
    sent(agb, 3)
    pl.when(c == 1)(lambda: sent(hx, 0))
    sent(tb.at[pl.ds(0, margin)], 1)
    sent(mrc.at[pl.ds(0, GROUP - 1)], 4)
    arrived(arcv2.at[pl.ds(0, 7)], 7)
    ar2src[...] = jnp.sum(arcv2[...], axis=0)
    for dz, dy in near:
        send(ar2src, arcv.at[me], 7, zpeer(dz, dy)[2], 8)
    arcv[me] = ar2src[...]
    arrived(grcv.at[pl.ds(0, GROUP - 1)], 6)

    def subtract(pz, carry):
        parts = [grcv[pz * NY + py].astype(F32) for py in range(NY)]
        for j in range(FR):
            science = None
            for py in range(NY):
                turn = (FL * (py - j)) % PW
                moved = pltpu.roll(parts[py], turn, 1) if turn else parts[py]
                turn = (FL * (py - FR)) % PW
                rest = parts[py][8 * j:8 * j + 8]
                rest = pltpu.roll(rest, turn, 1) if turn else rest
                moved = jnp.concatenate([moved, rest], axis=0)
                science = moved if science is None else jnp.where(lane32 >= FL * py, moved, science)
            r = rows_of(pz) * FR + j
            value = jnp.where(live, science - matched[r], 0.0)
            diffs[r] = value
            db[dmargin + r] = value.astype(BF16)
        return carry

    lax.fori_loop(0, NZ, subtract, 0, unroll=4)
    send(db.at[pl.ds(dmargin + (1 - c) * (ROWS - dmargin), dmargin)], db.at[pl.ds(c * (ROWS + dmargin), dmargin)], 8, partner, 9)
    for q in range(CAP):
        pltpu.make_async_copy(diffs.at[:, q, :], difference.at[:, pl.ds(q * PW, PW)], local.at[2]).start()
    build_windows(db, dmargin, ROWS, dmargin, dwindows, 4)

    arrived(other_rows(db, dmargin, c), 9)
    build_windows(db, (1 - c) * (ROWS + dmargin), dmargin, dmargin, dwindows, 7)
    banded(dwindows, dbands, 4, 0, (DK + 1) // 8, total)

    def unpair_filtered(q, carry):
        at = pl.ds(pl.multiple_of(q * CAP, CAP), CAP)
        tf[2 * q] = total[at, 0:PW]
        tf[2 * q + 1] = total[at, PW:2 * PW]
        return carry

    lax.fori_loop(0, ROWS // 2, unpair_filtered, 0, unroll=6)
    for q in range(CAP):
        pltpu.make_async_copy(tf.at[:, q, :], significance.at[:, pl.ds(q * PW, PW)], local.at[3]).start()
    arrived(arcv.at[pl.ds(0, GROUP - 1)], 8)
    sums = jnp.sum(arcv[...], axis=0)
    whole_square = jnp.sum(jnp.where(lane1 == 0, sums, 0.0), axis=1, keepdims=True)
    whole_count = jnp.sum(jnp.where(lane1 == 1, sums, 0.0), axis=1, keepdims=True)
    level = whole_square / whole_count
    taps = detection_kernel[...].astype(F32)
    norm = jnp.sum(jnp.sum(taps * taps, axis=1, keepdims=True), axis=0, keepdims=True)
    second = lax.broadcasted_iota(I32, (8, PW), 0) == 1
    numbers[...] = jnp.where(second, 1.0 / jnp.sqrt(1.0 + level * norm), level)
    report = pltpu.make_async_copy(numbers, stats, local.at[4])
    report.start()
    sent(grcv.at[pl.ds(0, GROUP - 1)], 5)
    sent(arcv2.at[pl.ds(0, 7)], 6)
    sent(arcv.at[pl.ds(0, GROUP - 1)], 7)
    sent(db.at[pl.ds(0, dmargin)], 8)
    pltpu.make_async_copy(diffs, diffs, local.at[2]).wait()
    pltpu.make_async_copy(tf, tf, local.at[3]).wait()
    report.wait()


def other_rows(ref, margin, c):
    return ref.at[pl.ds((1 - c) * (ROWS + margin), margin)]


def finish_kernel(difference, filtered, stats, out_difference, out_significance, out_noise, held, sums, numbers, ins, outs):
    loads = [
        pltpu.make_async_copy(stats, numbers, ins.at[0]),
        pltpu.make_async_copy(filtered, sums, ins.at[1]),
        pltpu.make_async_copy(difference, held, ins.at[2]),
    ]
    stores = [
        pltpu.make_async_copy(numbers.at[pl.ds(0, 1)], out_noise, outs.at[0]),
        pltpu.make_async_copy(sums, out_significance, outs.at[1]),
        pltpu.make_async_copy(held, out_difference, outs.at[2]),
    ]
    for load in loads:
        load.start()
    loads[0].wait()
    stores[0].start()
    loads[1].wait()
    sums[...] = sums[...] * numbers[1:2, 0:1]
    stores[1].start()
    loads[2].wait()
    stores[2].start()
    for store in stores:
        store.wait()


def on_device(
    exposure, row_shift, row_fraction, column_shift, column_fraction, piece_width,
    route_tile, route_cell, template, match_kernel, detection_kernel,
):
    vmem = pl.BlockSpec(memory_space=pltpu.VMEM)
    far = pl.BlockSpec(memory_space=pl.ANY)
    wide = template.shape[2]
    margin, dmargin = KS // 2, DK // 2
    difference, filtered, stats = pl.pallas_call(
        kernel,
        out_shape=(
            jax.ShapeDtypeStruct((ROWS, wide), F32),
            jax.ShapeDtypeStruct((ROWS, wide), F32),
            jax.ShapeDtypeStruct((8, PW), F32),
        ),
        in_specs=[far, far, vmem, vmem] + [far] * 7,
        out_specs=(far, far, far),
        scratch_shapes=[
            pltpu.VMEM((ROWS + HALO, NP, PW), F32),
            pltpu.VMEM((HALO, NP, PW), F32),
            pltpu.VMEM((ROWS, CAP, PW), F32),
            pltpu.VMEM((ROWS + 2 * margin, CAP, PW), BF16),
            pltpu.VMEM((ROWS, 1, PW), F32),
            pltpu.VMEM((NP, PW), F32),
            pltpu.VMEM((NP, PW), F32),
            pltpu.VMEM((GROUP, NP, PW), BF16),
            pltpu.VMEM((GROUP, NP, PW), BF16),
            pltpu.VMEM((NX - 1, GROUP, NP, PW), BF16),
            pltpu.VMEM((GROUP * CAP, PW), F32),
            pltpu.VMEM((GROUP, ROWS, PW), BF16),
            pltpu.VMEM((GROUP, ROWS, PW), BF16),
            pltpu.VMEM((NY * CAP, PW), F32),
            pltpu.VMEM((GROUP, ROWS, PW), BF16),
            pltpu.VMEM((GROUP, ROWS, PW), BF16),
            pltpu.VMEM((GROUP, ROWS, PW), F32),
            pltpu.VMEM((48 * 8, PW), F32),
            pltpu.VMEM((48 * 8, PW), F32),
            pltpu.VMEM(((KS + 2) * 2 * PW, PW), BF16),
            pltpu.VMEM(((DK + 2) * 2 * PW, PW), BF16),
            pltpu.VMEM((2, (ROWS // 2 + margin) * CAP, 2 * PW), BF16),
            pltpu.VMEM((2, (ROWS // 2 + dmargin) * CAP, 2 * PW), BF16),
            pltpu.VMEM((ROWS // 2 * CAP, 2 * PW), F32),
            pltpu.VMEM((ROWS, CAP, PW), F32),
            pltpu.VMEM((ROWS, CAP, PW), F32),
            pltpu.VMEM((ROWS + 2 * dmargin, CAP, PW), BF16),
            pltpu.VMEM((1, PW), F32),
            pltpu.VMEM((GROUP, 1, PW), F32),
            pltpu.VMEM((1, PW), F32),
            pltpu.VMEM((8, 1, PW), F32),
            pltpu.VMEM((8, PW), F32),
            pltpu.SemaphoreType.DMA((13,)),
            pltpu.SemaphoreType.DMA((9,)),
            pltpu.SemaphoreType.DMA((17,)),
            pltpu.VMEM((1, ROWS), BF16),
            pltpu.VMEM((1, NP * PW), BF16),
            pltpu.VMEM((1, NP), I32),
            pltpu.VMEM((1, NP), I32),
            pltpu.VMEM((1, NP), I32),
            pltpu.VMEM((KS, KS), BF16),
            pltpu.VMEM((DK, DK), BF16),
        ],
        compiler_params=pltpu.CompilerParams(collective_id=0, has_side_effects=True, vmem_limit_bytes=60 * 1024 * 1024),
        name="warp_match_detect",
    )(
        exposure[0], template[0], row_shift, column_shift, row_fraction, column_fraction,
        piece_width, route_tile, route_cell, match_kernel[0], detection_kernel[0],
    )
    difference, significance, noise = pl.pallas_call(
        finish_kernel,
        out_shape=(
            jax.ShapeDtypeStruct((ROWS, wide), F32),
            jax.ShapeDtypeStruct((ROWS, wide), F32),
            jax.ShapeDtypeStruct((1, PW), F32),
        ),
        in_specs=[far] * 3,
        out_specs=(far, far, far),
        scratch_shapes=[
            pltpu.VMEM((ROWS, wide), F32),
            pltpu.VMEM((ROWS, wide), F32),
            pltpu.VMEM((8, PW), F32),
            pltpu.SemaphoreType.DMA((3,)),
            pltpu.SemaphoreType.DMA((3,)),
        ],
        compiler_params=pltpu.CompilerParams(vmem_limit_bytes=60 * 1024 * 1024),
        name="finish",
    )(difference, filtered, stats)
    return difference[None], significance[None], noise[0, 0]


def solution(mesh):
    finer = Mesh(
        mesh.devices.reshape(NZ, NX, NY, mesh.shape["row"]), ("ccd_0", "ccd_1", "ccd_2", "row")
    )
    placed = (
        P(CCD, "row", None),
        P(CCD),
        P(CCD, "row"),
        P(CCD),
        P(CCD, None),
        P(CCD, None),
        P(CCD, None),
        P(CCD, None),
        P(CCD, "row", None),
        P(CCD, None, None),
        P(CCD, None, None),
    )
    return jax.shard_map(
        on_device,
        mesh=finer,
        in_specs=placed,
        out_specs=(P(CCD, "row", None), P(CCD, "row", None), P()),
        check_vma=False,
    )
```
